256 devices in a mesh: grp: 8 (over x, core), dev: 32 (over z, y).
Axes of the slice: x: 4, y: 4, z: 8, core: 2. Of those that a mesh axis runs over, the one named last changes fastest.
Arguments:
- points: bfloat16 [524288, 1024], P(('grp', 'dev')), may hold values from -6 to 6
- blocks: int32 [524288, 1], P(('grp', 'dev')), may hold values from 0 to 255; in each aligned block of 2048 rows (0 to 2047, 2048 to 4095, ...) at most 16 rows name the same one
- finals: int32 [524288], P(('grp', 'dev')), may hold values from 0 to 255
- centroids: bfloat16 [65536, 1024], P('dev'), may hold values from -6 to 6
Outputs:
- distances: bfloat16 [524288, 256], P(('grp', 'dev'))
- refreshed_centroids: float32 [65536, 1024], P('dev', 'grp')
The draws below stay inside these ranges and needn't reach their ends.
Inputs may be any that keep to these rules, and one draw needn't show every extreme that they name: `blocks`: among the 2048 rows of one device no block is named by more than 16 rows, and some block by exactly 16. Block b is held by index b // 8 of dev. The point's centroid is row 256 * blocks + finals of centroids.
All inputs are finite; a program needn't handle non-finite values.
Results may differ from the reference program's by a relative error of at most 0.008.
Values may be sent and summed in bfloat16 or wider, within the bound.
No kernel may reach another device: no remote copies, remote signals or barrier semaphores. Data moves between devices by JAX's collectives and lax.ppermute only.
A program may use at most 128 MiB of HBM per device.

```python
import math
import jax
import jax.numpy as jnp
import numpy as np
from jax import lax

D = 1024
BS = 256
POINTS_PER_SHARD = 2048
NB = 256
K = 65536
P_SIZE = 524288
MOST = 16
N_GRP = 8
N_DEV = 32


def place_ends(entries, own_key, smallest, top_value):
    dims = entries.shape
    index_at = [jax.random.randint(jax.random.fold_in(own_key, axis), (), 0, dims[axis]) for axis in range(len(dims))]
    entries = entries.at[tuple(index_at)].set(smallest)
    longest = dims.index(max(dims))
    index_at[longest] = (index_at[longest] + 1) % dims[longest]
    return entries.at[tuple(index_at)].set(top_value)


def shard_levels(stream_key, extent, cuts, smallest, top_value):
    def one(position, blocks):
        steps = jax.random.uniform(jax.random.fold_in(jax.random.fold_in(stream_key, 6), position), (blocks,), jnp.float32, smallest / len(cuts), top_value / len(cuts))
        return jnp.repeat(jnp.exp(steps), extent[position] // blocks).reshape((-1,) + (1,) * (len(extent) - position - 1))

    loudness = one(*cuts[0])
    for cut in cuts[1:]:
        loudness = loudness * one(*cut)
    return loudness


def assign_block(key, own, number, rows, count, top, most, skew):
    ranking = jax.random.permutation(key, count)
    heavy_load, usual = load_shares(count, rows * top, most, skew, True), load_shares(count, rows * top, most, skew, False)
    places = jnp.arange(count)

    def named(sizes, offset_by):
        used = int((sizes > 0).sum())
        fixed = max(1, used // 4)
        shifted = fixed + (places - fixed + offset_by * (used - fixed)) % max(1, count - fixed)
        return jnp.zeros((count,), jnp.int32).at[ranking[jnp.where(places < fixed, places, shifted)]].set(jnp.asarray(sizes, jnp.int32))

    sizes = jnp.where(number % 4 == 0, named(heavy_load, number // 4), named(usual, number - number // 4 - 1))
    mixed = jax.random.permutation(jax.random.fold_in(own, 3), count)
    giver, taker = mixed[0:count // 2 * 2:2], mixed[1:count // 2 * 2:2]
    margin = jnp.minimum(sizes[giver] - 1, most - sizes[taker]) // 2
    margin = jnp.where((giver == ranking[0]) | (taker == ranking[0]) | (sizes[taker] == 0), 0, jnp.maximum(margin, 0))
    shifted = jax.random.randint(jax.random.fold_in(own, 4), (count // 2,), 0, 1 << 20) % (margin + 1)
    sizes = sizes.at[giver].add(-shifted).at[taker].add(shifted)
    items = jnp.searchsorted(jnp.cumsum(sizes), jnp.arange(rows * top), side="right").astype(jnp.int32)
    grid = items.reshape(top, rows).T
    grid = grid[jax.random.permutation(jax.random.fold_in(own, 1), rows)]
    offset_by = jax.random.randint(jax.random.fold_in(own, 2), (rows, 1), 0, top)
    return jnp.take_along_axis(grid, (jnp.arange(top)[None, :] + offset_by) % top, axis=1)


def load_shares(amount, total, limit, slope, full):
    loads = [(1 << 20) // math.isqrt(rank ** slope) + 1 for rank in range(1, amount + 1)]
    largest = limit if full else min(limit, max(-(-total // amount), total * loads[0] // sum(loads)))
    least = 1 if total - largest >= amount - 1 else 0
    holding, surplus = [largest] + [least] * (amount - 1), total - largest - least * (amount - 1)
    while surplus > 0:
        free = [i for i in range(1, amount) if holding[i] < largest] or [i for i in range(1, amount) if holding[i] < limit]
        mass, left = sum([loads[i] for i in free]), surplus
        for i in free:
            extra = min(limit - holding[i], max(1, left * loads[i] // mass), surplus)
            holding[i] = holding[i] + extra
            surplus = surplus - extra
    return np.array(holding)


def normal_values(stream_key, dims, scale, bound, pieces=(), held_as=jnp.bfloat16):
    gain = shard_levels(stream_key, dims, pieces, -0.22, 0.18) if pieces else 1.0
    values = jax.random.normal(stream_key, dims, jnp.float32) * scale * gain
    return jnp.minimum(jnp.maximum(values, -bound), bound).astype(held_as)


def setup_inputs(seed: int = 0) -> dict:
    key_list = jax.random.split(jax.random.key(seed), 5)
    points = normal_values(key_list[0], (P_SIZE, D), 1.0, 6.0, ((0, 256),))
    blocks_keys = jax.random.split(jax.random.fold_in(key_list[1], 1), P_SIZE // POINTS_PER_SHARD)
    blocks_turns = jax.random.permutation(jax.random.fold_in(key_list[1], 3), P_SIZE // POINTS_PER_SHARD)
    blocks = jax.vmap(lambda own, number: assign_block(jax.random.fold_in(key_list[1], 2), own, number, POINTS_PER_SHARD, NB, 1, MOST, 2))(blocks_keys, blocks_turns).reshape((P_SIZE, 1))
    finals = place_ends(jax.random.randint(key_list[2], (P_SIZE,), 0, BS), jax.random.fold_in(key_list[2], 1), 0, BS - 1).astype(jnp.int32)
    centroids = normal_values(key_list[3], (K, D), 1.0, 6.0, ((0, 32),))
    return {"points": points, "blocks": blocks, "finals": finals, "centroids": centroids}


def reference(points, blocks, finals, centroids):
    npoints, width = points.shape
    nblocks = centroids.shape[0] // BS
    reach = N_GRP * N_DEV * MOST
    block_ids = blocks[:, 0].astype(jnp.int32)
    order = jnp.argsort(block_ids, stable=True).astype(jnp.int32)
    ordered = block_ids[order]
    labels = jnp.arange(nblocks, dtype=jnp.int32)
    starts = jnp.searchsorted(ordered, labels, side="left").astype(jnp.int32)
    stops = jnp.searchsorted(ordered, labels, side="right").astype(jnp.int32)
    padded = jnp.concatenate([order, jnp.zeros((reach,), jnp.int32)])
    columns = jnp.arange(BS, dtype=jnp.int32)
    positions = jnp.arange(reach, dtype=jnp.int32)

    def one_block(label):
        begin = starts[label]
        chosen = lax.dynamic_slice_in_dim(padded, begin, reach)
        live = positions < (stops[label] - begin)
        rows = points[chosen].astype(jnp.float32)
        centroid_table = lax.dynamic_slice_in_dim(centroids, (label * BS).astype(jnp.int32), BS, 0).astype(jnp.float32)
        cross_products = jnp.dot(rows, centroid_table.T, preferred_element_type=jnp.float32)
        dists = (jnp.sum(rows * rows, axis=1)[:, None] - 2.0 * cross_products + jnp.sum(centroid_table * centroid_table, axis=1)[None, :]) / width
        onehot_assign = jnp.where(live[:, None] & (finals[chosen][:, None] == columns[None, :]), 1.0, 0.0).astype(jnp.float32)
        sums = jnp.dot(onehot_assign.T, rows, preferred_element_type=jnp.float32)
        counts = jnp.sum(onehot_assign, axis=0)
        fresh = (sums + centroid_table) / (counts + 1.0)[:, None]
        where_to = jnp.where(live, chosen, npoints).astype(jnp.int32)
        return dists.astype(jnp.bfloat16), where_to, fresh

    dists, where_to, fresh = lax.map(one_block, labels)
    table = jnp.zeros((npoints + 1, BS), jnp.bfloat16).at[where_to.reshape(-1)].set(dists.reshape(-1, BS))
    return table[:npoints], fresh.reshape(nblocks * BS, width)
```

```python
import functools

import jax
import jax.numpy as jnp
from jax import lax
from jax.experimental import pallas as pl
from jax.experimental.pallas import tpu as pltpu
from jax.sharding import Mesh
from jax.sharding import PartitionSpec as P

BS = 256
MOST = 16
NX, NC, NZ, NY = 4, 2, 8, 4
NG = NX * NC
NB = NZ * NY * NG
DESTS = NG * NY
SLOTS = NZ * MOST
WIDTHS = (512, 512)
PLANE = ("x", "c", "y")
PER_STEP = 4
F32, BF16 = jnp.float32, jnp.bfloat16


def nt_dot(a, b):
    return lax.dot_general(a, b, (((1,), (1,)), ((), ())), preferred_element_type=F32)


def tn_dot(a, b):
    return lax.dot_general(a, b, (((0,), (0,)), ((), ())), preferred_element_type=F32)


def slots_of(block_row):
    npts = block_row.shape[1]
    piece = 128
    before = (
        lax.broadcasted_iota(jnp.int32, (piece, piece), 0)
        < lax.broadcasted_iota(jnp.int32, (piece, piece), 1)
    ).astype(BF16)
    carry = jnp.zeros((NB, 1), F32)
    ranks = []
    for i in range(npts // piece):
        part = block_row[:, i * piece : (i + 1) * piece]
        member = lax.broadcasted_iota(jnp.int32, (NB, piece), 0) == part
        ones = jnp.where(member, 1.0, 0.0)
        seen = jnp.dot(ones.astype(BF16), before, preferred_element_type=F32) + carry
        ranks.append(jnp.sum(ones * seen, axis=0, keepdims=True))
        carry = carry + jnp.sum(ones, axis=1, keepdims=True)
    rank = jnp.concatenate(ranks, axis=1).astype(jnp.int32)
    zz = block_row // (NY * NG)
    yy = (block_row // NG) % NY
    gg = block_row % NG
    return ((gg * NY + yy) * NZ + zz) * MOST + rank


def first_prep(block_ref, final_ref, points_ref, out_ref, slot_ref, target_ref, slots):
    step = pl.program_id(0)

    @pl.when(step == 0)
    def _():
        found = slots_of(block_ref[...])
        slots[...] = found
        slot_ref[...] = found

    rows = PER_STEP * SLOTS
    npts = points_ref.shape[0]
    at = step * rows + lax.broadcasted_iota(jnp.int32, (rows, npts), 0)
    pick = jnp.where(at == slots[...], 1.0, 0.0).astype(BF16)
    moved = jnp.dot(pick, points_ref[...], preferred_element_type=F32)
    out_ref[...] = moved.astype(BF16).reshape(out_ref.shape)
    marks = jnp.broadcast_to((final_ref[...] + 1).astype(F32).astype(BF16), (8, npts))
    target = nt_dot(marks, pick)[0:1] - 1.0
    target_ref[...] = target.astype(jnp.int32).reshape(target_ref.shape)


def later_prep(slot_ref, points_ref, out_ref):
    step = pl.program_id(0)
    rows = PER_STEP * SLOTS
    npts = points_ref.shape[0]
    at = step * rows + lax.broadcasted_iota(jnp.int32, (rows, npts), 0)
    pick = jnp.where(at == slot_ref[...], 1.0, 0.0).astype(BF16)
    moved = jnp.dot(pick, points_ref[...], preferred_element_type=F32)
    out_ref[...] = moved.astype(BF16).reshape(out_ref.shape)


def prepare(block_row, final_row, points, start, width, slot_row):
    npts = points.shape[0]
    steps = DESTS // PER_STEP
    column = start // width
    whole = pl.BlockSpec((1, npts), lambda i: (0, 0))
    point_spec = pl.BlockSpec((npts, width), lambda i: (0, column))
    out_spec = pl.BlockSpec((PER_STEP, SLOTS, width), lambda i: (i, 0, 0))
    out_shape = jax.ShapeDtypeStruct((DESTS, SLOTS, width), BF16)
    cost = pl.CostEstimate(
        flops=2 * DESTS * SLOTS * npts * width,
        bytes_accessed=2 * width * (npts + DESTS * SLOTS),
        transcendentals=0,
    )
    if slot_row is not None:
        return pl.pallas_call(
            later_prep,
            grid=(steps,),
            in_specs=[whole, point_spec],
            out_specs=out_spec,
            out_shape=out_shape,
            cost_estimate=cost,
        )(slot_row, points)
    return pl.pallas_call(
        first_prep,
        grid=(steps,),
        in_specs=[whole, whole, point_spec],
        out_specs=(
            out_spec,
            whole,
            pl.BlockSpec((1, 1, PER_STEP * SLOTS), lambda i: (i, 0, 0)),
        ),
        out_shape=(
            out_shape,
            jax.ShapeDtypeStruct((1, npts), jnp.int32),
            jax.ShapeDtypeStruct((steps, 1, PER_STEP * SLOTS), jnp.int32),
        ),
        scratch_shapes=[pltpu.VMEM((1, npts), jnp.int32)],
        cost_estimate=cost,
    )(block_row, final_row, points)


def work_kernel(first, last, *refs):
    refs = list(refs)
    rows_ref, cent_ref, target_ref = refs[:3]
    part_ref = None if first else refs[3]
    sums_ref, result_ref = refs[-2:]
    rows = rows_ref[...].reshape(DESTS * MOST, rows_ref.shape[-1])
    table = cent_ref[0]
    onehot = jnp.where(
        lax.broadcasted_iota(jnp.int32, (BS, DESTS * MOST), 0) == target_ref[0], 1.0, 0.0
    ).astype(BF16)
    sums = jnp.dot(onehot, rows, preferred_element_type=F32)
    sums_ref[0, 0:BS] = sums.astype(BF16)
    if first:
        ones = jnp.ones((8, DESTS * MOST), BF16)
        count = nt_dot(ones, onehot)
        high = jnp.floor(count * (1.0 / 16.0))
        low = count - 16.0 * high
        which = lax.broadcasted_iota(jnp.int32, count.shape, 0)
        digits = jnp.where(which == 0, low, jnp.where(which == 1, high, 0.0))
        extra = sums_ref.shape[-1] - BS
        sums_ref[0, BS : BS + 8, 0:BS] = digits.astype(BF16)
        if extra:
            sums_ref[0, BS : BS + 8, BS:] = jnp.zeros((8, extra), BF16)
    cross = nt_dot(rows, table)
    wide = rows.astype(F32)
    row_norm = jnp.sum(wide * wide, axis=1, keepdims=True)
    tall = table.astype(F32)
    cent_norm = jnp.sum(tall * tall, axis=1, keepdims=True)
    cent_norm = jnp.transpose(jnp.broadcast_to(cent_norm, (BS, 128)))[0:1]
    total = row_norm - 2.0 * cross + cent_norm
    if not first:
        total = total + part_ref[0]
    if last:
        result_ref[...] = (total * (1.0 / 1024.0)).astype(BF16).reshape(result_ref.shape)
    else:
        result_ref[0] = total


def block_work(rows, table, target, part, start, last):
    width = rows.shape[-1]
    first = part is None
    taken = DESTS * MOST
    tall = BS + 8 if first else BS
    row_spec = pl.BlockSpec((DESTS, MOST, width), lambda j: (0, j, 0))
    part_spec = pl.BlockSpec((1, taken, BS), lambda j: (j, 0, 0))
    in_specs = [
        row_spec,
        pl.BlockSpec((1, BS, width), lambda j: (j, 0, start // width)),
        pl.BlockSpec((1, 1, taken), lambda j: (j, 0, 0)),
    ]
    operands = [rows, table, target]
    if not first:
        in_specs.append(part_spec)
        operands.append(part)
    if last:
        result_spec = pl.BlockSpec((DESTS, MOST, BS), lambda j: (0, j, 0))
        result_shape = jax.ShapeDtypeStruct((DESTS, SLOTS, BS), BF16)
    else:
        result_spec = part_spec
        result_shape = jax.ShapeDtypeStruct((NZ, taken, BS), F32)
    return pl.pallas_call(
        functools.partial(work_kernel, first, last),
        grid=(NZ,),
        in_specs=in_specs,
        out_specs=(pl.BlockSpec((1, tall, width), lambda j: (j, 0, 0)), result_spec),
        out_shape=(jax.ShapeDtypeStruct((NZ, tall, width), BF16), result_shape),
        cost_estimate=pl.CostEstimate(
            flops=4 * NZ * taken * BS * width,
            bytes_accessed=2 * width * NZ * (taken + 2 * BS) + 8 * NZ * taken * BS,
            transcendentals=0,
        ),
    )(*operands)


def return_kernel(slot_ref, returned_ref, out_ref):
    rows = out_ref.shape[0]
    total = returned_ref.shape[0]
    slot = jnp.broadcast_to(slot_ref[...].astype(F32), (128, rows))
    column = jnp.transpose(slot)[:, 0:1].astype(jnp.int32)
    pick = jnp.where(
        lax.broadcasted_iota(jnp.int32, (rows, total), 1) == column, 1.0, 0.0
    ).astype(BF16)
    got = jnp.dot(pick, returned_ref[...], preferred_element_type=F32)
    out_ref[...] = got.astype(BF16)


def pick_back(slot_row, returned):
    npts = slot_row.shape[1]
    rows = 256
    return pl.pallas_call(
        return_kernel,
        grid=(npts // rows,),
        in_specs=[
            pl.BlockSpec((1, rows), lambda i: (0, i)),
            pl.BlockSpec(returned.shape, lambda i: (0, 0)),
        ],
        out_specs=pl.BlockSpec((rows, BS), lambda i: (i, 0)),
        out_shape=jax.ShapeDtypeStruct((npts, BS), BF16),
        cost_estimate=pl.CostEstimate(
            flops=2 * npts * returned.shape[0] * BS,
            bytes_accessed=2 * BS * (npts + returned.shape[0]),
            transcendentals=0,
        ),
    )(slot_row, returned)


def exchange(values, axes):
    return lax.all_to_all(values, axes, split_axis=0, concat_axis=0, tiled=True)


def shards(points, blocks, finals, centroids):
    npts, width = points.shape
    group = lax.axis_index("x") * NC + lax.axis_index("c")
    own = lax.dynamic_slice_in_dim(centroids, group * BS, BS, 0)
    table = lax.all_gather(own, "z", axis=0, tiled=False)

    block_row = blocks.reshape(1, npts)
    final_row = finals.reshape(1, npts)
    slot_row = None
    arrived, start = [], 0
    for size in WIDTHS:
        if slot_row is None:
            sent, slot_row, target = prepare(block_row, final_row, points, start, size, None)
            arrived.append(exchange(sent, PLANE))
            target = exchange(target.reshape(DESTS, SLOTS), PLANE)
            target = jnp.transpose(target.reshape(DESTS, NZ, MOST), (1, 0, 2))
            target = target.reshape(NZ, 1, DESTS * MOST)
        else:
            sent = prepare(block_row, final_row, points, start, size, slot_row)
            arrived.append(exchange(sent, PLANE))
        start += size

    part, start, shares = None, 0, []
    for i, size in enumerate(WIDTHS):
        sums, part = block_work(arrived[i], table, target, part, start, i == len(WIDTHS) - 1)
        shares.append(lax.psum_scatter(sums, "z", scatter_dimension=0, tiled=True)[0])
        start += size
    returned = exchange(part, PLANE).reshape(DESTS * SLOTS, BS)
    distances = pick_back(slot_row, returned)

    counts = shares[0][BS, :BS].astype(F32) + 16.0 * shares[0][BS + 1, :BS].astype(F32)
    total = jnp.concatenate([s[:BS].astype(F32) for s in shares], axis=1)
    fresh = (total + own.astype(F32)) / (counts + 1.0)[:, None]
    fresh = lax.all_to_all(fresh.astype(BF16), ("x", "c"), split_axis=1, concat_axis=0, tiled=True)
    return distances, fresh.astype(F32)


def solution(mesh):
    split = Mesh(mesh.devices.reshape(NX, NC, NZ, NY), ("x", "c", "z", "y"))
    every = ("x", "c", "z", "y")
    placed = (P(every, None), P(every, None), P(every), P(("z", "y"), None))
    return jax.shard_map(
        shards,
        mesh=split,
        in_specs=placed,
        out_specs=(P(every, None), P(("z", "y"), ("x", "c"))),
        check_vma=False,
    )
```

```python
import functools

import jax
import jax.numpy as jnp
from jax import lax
from jax.experimental import pallas as pl
from jax.experimental.pallas import tpu as pltpu
from jax.sharding import Mesh
from jax.sharding import PartitionSpec as P

BS = 256
MOST = 16
NX, NC, NZ, NY = 4, 2, 8, 4
NG = NX * NC
NB = NZ * NY * NG
DESTS = NG * NY
SLOTS = NZ * MOST
WIDTHS = (512, 512)
PLANE = ("x", "c", "y")
PER_STEP = 4
F32, BF16 = jnp.float32, jnp.bfloat16


def nt_dot(a, b):
    return lax.dot_general(a, b, (((1,), (1,)), ((), ())), preferred_element_type=F32)


def slots_of(block_row):
    npts = block_row.shape[1]
    piece = 128
    before = (
        lax.broadcasted_iota(jnp.int32, (piece, piece), 0)
        < lax.broadcasted_iota(jnp.int32, (piece, piece), 1)
    ).astype(BF16)
    carry = jnp.zeros((NB, 1), F32)
    ranks = []
    for i in range(npts // piece):
        part = block_row[:, i * piece : (i + 1) * piece]
        member = lax.broadcasted_iota(jnp.int32, (NB, piece), 0) == part
        ones = jnp.where(member, 1.0, 0.0)
        seen = jnp.dot(ones.astype(BF16), before, preferred_element_type=F32) + carry
        ranks.append(jnp.sum(ones * seen, axis=0, keepdims=True))
        carry = carry + jnp.sum(ones, axis=1, keepdims=True)
    rank = jnp.concatenate(ranks, axis=1).astype(jnp.int32)
    zz = block_row // (NY * NG)
    yy = (block_row // NG) % NY
    gg = block_row % NG
    return ((gg * NY + yy) * NZ + zz) * MOST + rank


def pick_rows(slots, base, rows):
    npts = slots.shape[1]
    tall = 256
    lane = 128
    line = lax.broadcasted_iota(jnp.int32, (tall, lane), 0).astype(F32).astype(BF16)
    parts = []
    for i in range(rows // tall):
        local = slots - (base + i * tall)
        local = jnp.where((local >= 0) & (local < tall), local, -1).astype(F32).astype(BF16)
        parts.append(
            jnp.concatenate(
                [
                    jnp.where(line == local[:, k : k + lane], 1.0, 0.0).astype(BF16)
                    for k in range(0, npts, lane)
                ],
                axis=1,
            )
        )
    return jnp.concatenate(parts, axis=0)


def first_prep(block_ref, final_ref, points_ref, out_ref, slot_ref, slots):
    step = pl.program_id(0)

    @pl.when(step == 0)
    def _():
        found = slots_of(block_ref[...])
        slots[...] = found
        slot_ref[...] = found

    rows = PER_STEP * SLOTS
    npts, width = points_ref.shape
    pick = pick_rows(slots[...], step * rows, rows)
    moved = jnp.dot(pick, points_ref[...], preferred_element_type=F32)
    out_ref[:, 0:SLOTS] = moved.astype(BF16).reshape(PER_STEP, SLOTS, width)
    marks = jnp.broadcast_to((final_ref[...] + 1).astype(F32).astype(BF16), (8, npts))
    target = nt_dot(marks, pick).astype(BF16)
    blank = jnp.zeros((8, width - SLOTS), BF16)
    for i in range(PER_STEP):
        one = target[:, i * SLOTS : (i + 1) * SLOTS]
        out_ref[i, SLOTS : SLOTS + 8] = jnp.concatenate([one, blank], axis=1)


def later_prep(slot_ref, points_ref, out_ref):
    rows = PER_STEP * SLOTS
    pick = pick_rows(slot_ref[...], pl.program_id(0) * rows, rows)
    moved = jnp.dot(pick, points_ref[...], preferred_element_type=F32)
    out_ref[...] = moved.astype(BF16).reshape(out_ref.shape)


def prepare(block_row, final_row, points, start, width, slot_row):
    npts = points.shape[0]
    steps = DESTS // PER_STEP
    column = start // width
    whole = pl.BlockSpec((1, npts), lambda i: (0, 0))
    point_spec = pl.BlockSpec((npts, width), lambda i: (0, column))
    tall = SLOTS if slot_row is not None else SLOTS + 8
    out_spec = pl.BlockSpec((PER_STEP, tall, width), lambda i: (i, 0, 0))
    out_shape = jax.ShapeDtypeStruct((DESTS, tall, width), BF16)
    cost = pl.CostEstimate(
        flops=2 * DESTS * SLOTS * npts * width,
        bytes_accessed=2 * width * (npts + DESTS * SLOTS),
        transcendentals=0,
    )
    if slot_row is not None:
        return pl.pallas_call(
            later_prep,
            grid=(steps,),
            in_specs=[whole, point_spec],
            out_specs=out_spec,
            out_shape=out_shape,
            cost_estimate=cost,
        )(slot_row, points)
    return pl.pallas_call(
        first_prep,
        grid=(steps,),
        in_specs=[whole, whole, point_spec],
        out_specs=(out_spec, whole),
        out_shape=(out_shape, jax.ShapeDtypeStruct((1, npts), jnp.int32)),
        scratch_shapes=[pltpu.VMEM((1, npts), jnp.int32)],
        cost_estimate=cost,
    )(block_row, final_row, points)


def work_kernel(first, last, *refs):
    refs = list(refs)
    rows_ref, cent_ref, target_ref = refs[:3]
    part_ref = None if first else refs[3]
    sums_ref, result_ref = refs[-2:]
    rows = rows_ref[...].reshape(DESTS * MOST, rows_ref.shape[-1])
    table = cent_ref[0]
    onehot = jnp.where(
        lax.broadcasted_iota(jnp.int32, (BS, DESTS * MOST), 0) == target_ref[0], 1.0, 0.0
    ).astype(BF16)
    sums = jnp.dot(onehot, rows, preferred_element_type=F32)
    sums_ref[0, 0:BS] = sums.astype(BF16)
    if first:
        ones = jnp.ones((8, DESTS * MOST), BF16)
        count = nt_dot(ones, onehot)
        high = jnp.floor(count * (1.0 / 16.0))
        low = count - 16.0 * high
        which = lax.broadcasted_iota(jnp.int32, count.shape, 0)
        digits = jnp.where(which == 0, low, jnp.where(which == 1, high, 0.0))
        extra = sums_ref.shape[-1] - BS
        sums_ref[0, BS : BS + 8, 0:BS] = digits.astype(BF16)
        if extra:
            sums_ref[0, BS : BS + 8, BS:] = jnp.zeros((8, extra), BF16)
    cross = nt_dot(rows, table)
    wide = rows.astype(F32)
    row_norm = jnp.sum(wide * wide, axis=1, keepdims=True)
    tall = table.astype(F32)
    cent_norm = jnp.sum(tall * tall, axis=1, keepdims=True)
    cent_norm = jnp.transpose(jnp.broadcast_to(cent_norm, (BS, 128)))[0:1]
    total = row_norm - 2.0 * cross + cent_norm
    if not first:
        total = total + part_ref[0]
    if last:
        result_ref[...] = (total * (1.0 / 1024.0)).astype(BF16).reshape(result_ref.shape)
    else:
        result_ref[0] = total


def block_work(rows, table, target, part, start, last):
    width = rows.shape[-1]
    first = part is None
    taken = DESTS * MOST
    tall = BS + 8 if first else BS
    row_spec = pl.BlockSpec((DESTS, MOST, width), lambda j: (0, j, 0))
    part_spec = pl.BlockSpec((1, taken, BS), lambda j: (j, 0, 0))
    in_specs = [
        row_spec,
        pl.BlockSpec((1, BS, width), lambda j: (j, 0, start // width)),
        pl.BlockSpec((1, 1, taken), lambda j: (j, 0, 0)),
    ]
    operands = [rows, table, target]
    if not first:
        in_specs.append(part_spec)
        operands.append(part)
    if last:
        result_spec = pl.BlockSpec((DESTS, MOST, BS), lambda j: (0, j, 0))
        result_shape = jax.ShapeDtypeStruct((DESTS, SLOTS, BS), BF16)
    else:
        result_spec = part_spec
        result_shape = jax.ShapeDtypeStruct((NZ, taken, BS), F32)
    return pl.pallas_call(
        functools.partial(work_kernel, first, last),
        grid=(NZ,),
        in_specs=in_specs,
        out_specs=(pl.BlockSpec((1, tall, width), lambda j: (j, 0, 0)), result_spec),
        out_shape=(jax.ShapeDtypeStruct((NZ, tall, width), BF16), result_shape),
        cost_estimate=pl.CostEstimate(
            flops=4 * NZ * taken * BS * width,
            bytes_accessed=2 * width * NZ * (taken + 2 * BS) + 8 * NZ * taken * BS,
            transcendentals=0,
        ),
    )(*operands)


def return_kernel(slot_ref, returned_ref, out_ref):
    rows = out_ref.shape[0]
    total = returned_ref.shape[0]
    slot = jnp.broadcast_to(slot_ref[...].astype(F32), (128, rows))
    column = jnp.transpose(slot)[:, 0:1].astype(jnp.int32)
    pick = jnp.where(
        lax.broadcasted_iota(jnp.int32, (rows, total), 1) == column, 1.0, 0.0
    ).astype(BF16)
    got = jnp.dot(pick, returned_ref[...], preferred_element_type=F32)
    out_ref[...] = got.astype(BF16)


def pick_back(slot_row, returned):
    npts = slot_row.shape[1]
    rows = 256
    return pl.pallas_call(
        return_kernel,
        grid=(npts // rows,),
        in_specs=[
            pl.BlockSpec((1, rows), lambda i: (0, i)),
            pl.BlockSpec(returned.shape, lambda i: (0, 0)),
        ],
        out_specs=pl.BlockSpec((rows, BS), lambda i: (i, 0)),
        out_shape=jax.ShapeDtypeStruct((npts, BS), BF16),
        cost_estimate=pl.CostEstimate(
            flops=2 * npts * returned.shape[0] * BS,
            bytes_accessed=2 * BS * (npts + returned.shape[0]),
            transcendentals=0,
        ),
    )(slot_row, returned)


def exchange(values, axes):
    return lax.all_to_all(values, axes, split_axis=0, concat_axis=0, tiled=True)


def shards(points, blocks, finals, centroids):
    npts, _ = points.shape
    group = lax.axis_index("x") * NC + lax.axis_index("c")
    own = lax.dynamic_slice_in_dim(centroids, group * BS, BS, 0)
    table = lax.all_gather(own, "z", axis=0, tiled=False)

    block_row = blocks.reshape(1, npts)
    final_row = finals.reshape(1, npts)
    low, high = WIDTHS
    sent, slot_row = prepare(block_row, final_row, points, 0, low, None)
    here = exchange(sent, PLANE)
    later = prepare(block_row, final_row, points, low, high, slot_row)
    here, later = lax.optimization_barrier((here, later))
    then = exchange(later, PLANE)

    target = here[:, SLOTS, :SLOTS].astype(jnp.int32) - 1
    target = jnp.transpose(target.reshape(DESTS, NZ, MOST), (1, 0, 2))
    target = target.reshape(NZ, 1, DESTS * MOST)
    sums, part = block_work(here, table, target, None, 0, False)
    share = lax.psum_scatter(sums, "z", scatter_dimension=0, tiled=True)[0]
    more, part = block_work(then, table, target, part, low, True)
    rest = lax.psum_scatter(more, "z", scatter_dimension=0, tiled=True)[0]
    returned = exchange(part, PLANE).reshape(DESTS * SLOTS, BS)
    distances = pick_back(slot_row, returned)
    distances, rest = lax.optimization_barrier((distances, rest))

    counts = share[BS, :BS].astype(F32) + 16.0 * share[BS + 1, :BS].astype(F32)
    total = jnp.concatenate([share[:BS].astype(F32), rest.astype(F32)], axis=1)
    fresh = (total + own.astype(F32)) / (counts + 1.0)[:, None]
    fresh = lax.all_to_all(fresh.astype(BF16), ("x", "c"), split_axis=1, concat_axis=0, tiled=True)
    return distances, fresh.astype(F32)


def solution(mesh):
    split = Mesh(mesh.devices.reshape(NX, NC, NZ, NY), ("x", "c", "z", "y"))
    every = ("x", "c", "z", "y")
    placed = (P(every, None), P(every, None), P(every), P(("z", "y"), None))
    return jax.shard_map(
        shards,
        mesh=split,
        in_specs=placed,
        out_specs=(P(every, None), P(("z", "y"), ("x", "c"))),
        check_vma=False,
    )
```

```python
import functools

import jax
import jax.numpy as jnp
from jax import lax
from jax.experimental import pallas as pl
from jax.experimental.pallas import tpu as pltpu
from jax.sharding import Mesh
from jax.sharding import PartitionSpec as P

BS = 256
MOST = 16
NX, NC, NZ, NY = 4, 2, 8, 4
NG = NX * NC
NB = NZ * NY * NG
DESTS = NG * NY
SLOTS = NZ * MOST
WIDTHS = (768, 256)
PLANE = ("x", "c", "y")
DIGIT = 64
PER_STEP = 4
F32, BF16 = jnp.float32, jnp.bfloat16


def nt_dot(a, b):
    return lax.dot_general(a, b, (((1,), (1,)), ((), ())), preferred_element_type=F32)


def slots_of(block_row):
    npts = block_row.shape[1]
    piece = 128
    row = lax.broadcasted_iota(jnp.int32, (piece, 2 * piece), 0)
    column = lax.broadcasted_iota(jnp.int32, (piece, 2 * piece), 1)
    before = jnp.where((row < column) | (column >= piece), 1.0, 0.0).astype(BF16)
    carry = jnp.zeros((NB, piece), F32)
    ranks = []
    for i in range(npts // piece):
        part = block_row[:, i * piece : (i + 1) * piece]
        member = lax.broadcasted_iota(jnp.int32, (NB, piece), 0) == part
        ones = jnp.where(member, 1.0, 0.0)
        seen = jnp.dot(ones.astype(BF16), before, preferred_element_type=F32)
        ranks.append(jnp.sum(ones * (seen[:, :piece] + carry), axis=0, keepdims=True))
        carry = carry + seen[:, piece:]
    rank = jnp.concatenate(ranks, axis=1).astype(jnp.int32)
    zz = block_row // (NY * NG)
    yy = (block_row // NG) % NY
    gg = block_row % NG
    return ((gg * NY + yy) * NZ + zz) * MOST + rank


def low_digits(slots):
    line = lax.broadcasted_iota(jnp.int32, (DIGIT, slots.shape[1]), 0)
    return jnp.where(line == slots % DIGIT, 1.0, 0.0).astype(BF16)


def pick_rows(slots, low, base, rows):
    npts = slots.shape[1]
    line = lax.broadcasted_iota(jnp.int32, (rows // DIGIT, npts), 0)
    high = jnp.where(line + base // DIGIT == slots // DIGIT, 1.0, 0.0)
    parts = []
    for i in range(rows // DIGIT):
        one = jnp.broadcast_to(high[i : i + 1], (16, npts)).astype(BF16)
        parts.append(low * jnp.concatenate([one] * (DIGIT // 16), axis=0))
    return jnp.concatenate(parts, axis=0)


def first_prep(block_ref, final_ref, points_ref, out_ref, slot_ref, slots, low):
    step = pl.program_id(0)

    @pl.when(step == 0)
    def _():
        found = slots_of(block_ref[...])
        slots[...] = found
        slot_ref[...] = found
        low[...] = low_digits(found)

    rows = PER_STEP * SLOTS
    npts, width = points_ref.shape
    pick = pick_rows(slots[...], low[...], step * rows, rows)
    moved = jnp.dot(pick, points_ref[...], preferred_element_type=F32)
    out_ref[:, 0:SLOTS] = moved.astype(BF16).reshape(PER_STEP, SLOTS, width)
    marks = jnp.broadcast_to((final_ref[...] + 1).astype(F32).astype(BF16), (8, npts))
    target = nt_dot(marks, pick).astype(BF16)
    blank = jnp.zeros((8, width - SLOTS), BF16)
    for i in range(PER_STEP):
        one = target[:, i * SLOTS : (i + 1) * SLOTS]
        out_ref[i, SLOTS : SLOTS + 8] = jnp.concatenate([one, blank], axis=1)


def later_prep(slot_ref, points_ref, out_ref, low):
    step = pl.program_id(0)

    @pl.when(step == 0)
    def _():
        low[...] = low_digits(slot_ref[...])

    rows = PER_STEP * SLOTS
    pick = pick_rows(slot_ref[...], low[...], step * rows, rows)
    moved = jnp.dot(pick, points_ref[...], preferred_element_type=F32)
    out_ref[...] = moved.astype(BF16).reshape(out_ref.shape)


def prepare(block_row, final_row, points, start, width, slot_row):
    npts = points.shape[0]
    steps = DESTS // PER_STEP
    column = start // width
    whole = pl.BlockSpec((1, npts), lambda i: (0, 0))
    point_spec = pl.BlockSpec((npts, width), lambda i: (0, column))
    tall = SLOTS if slot_row is not None else SLOTS + 8
    out_spec = pl.BlockSpec((PER_STEP, tall, width), lambda i: (i, 0, 0))
    out_shape = jax.ShapeDtypeStruct((DESTS, tall, width), BF16)
    cost = pl.CostEstimate(
        flops=2 * DESTS * SLOTS * npts * width,
        bytes_accessed=2 * width * (npts + DESTS * SLOTS),
        transcendentals=0,
    )
    if slot_row is not None:
        return pl.pallas_call(
            later_prep,
            grid=(steps,),
            in_specs=[whole, point_spec],
            out_specs=out_spec,
            out_shape=out_shape,
            scratch_shapes=[pltpu.VMEM((DIGIT, npts), BF16)],
            cost_estimate=cost,
        )(slot_row, points)
    return pl.pallas_call(
        first_prep,
        grid=(steps,),
        in_specs=[whole, whole, point_spec],
        out_specs=(out_spec, whole),
        out_shape=(out_shape, jax.ShapeDtypeStruct((1, npts), jnp.int32)),
        scratch_shapes=[pltpu.VMEM((1, npts), jnp.int32), pltpu.VMEM((DIGIT, npts), BF16)],
        cost_estimate=cost,
    )(block_row, final_row, points)


def work_kernel(first, me_ref, *refs):
    del me_ref
    place = pl.program_id(0)
    rows_ref, cent_ref, target_ref = refs[:3]
    rows = rows_ref[...].reshape(DESTS * MOST, rows_ref.shape[-1])
    table = cent_ref[0]
    onehot = jnp.where(
        lax.broadcasted_iota(jnp.int32, (BS, DESTS * MOST), 0) == target_ref[0], 1.0, 0.0
    ).astype(BF16)
    sums = jnp.dot(onehot, rows, preferred_element_type=F32).astype(BF16)
    cross = nt_dot(rows, table)
    wide = rows.astype(F32)
    row_norm = jnp.sum(wide * wide, axis=1, keepdims=True)
    tall = table.astype(F32)
    cent_norm = jnp.sum(tall * tall, axis=1, keepdims=True)
    cent_norm = jnp.transpose(jnp.broadcast_to(cent_norm, (BS, 128)))[0:1]
    total = row_norm - 2.0 * cross + cent_norm
    if first:
        sums_ref, result_ref = refs[3:]
        sums_ref[0, 0:BS] = sums
        ones = jnp.ones((8, DESTS * MOST), BF16)
        count = nt_dot(ones, onehot)
        high = jnp.floor(count * (1.0 / 16.0))
        low = count - 16.0 * high
        which = lax.broadcasted_iota(jnp.int32, count.shape, 0)
        digits = jnp.where(which == 0, low, jnp.where(which == 1, high, 0.0))
        blank = jnp.zeros((8, sums.shape[1] - BS), F32)
        digits = jnp.concatenate([digits, blank], axis=1)
        sums_ref[0, BS : BS + 8] = digits.astype(BF16)
        result_ref[0] = total
    else:
        part_ref, sum_refs, result_ref = refs[3], refs[4:-1], refs[-1]
        for i in range(NZ):

            @pl.when(place == i)
            def _(i=i):
                sum_refs[i][...] = sums

        total = (total + part_ref[0]) * (1.0 / 1024.0)
        result_ref[...] = total.astype(BF16).reshape(result_ref.shape)


def block_work(me, rows, table, target, part, start):
    width = rows.shape[-1]
    first = part is None
    taken = DESTS * MOST
    away = lambda k, me: lax.rem(me[0] - k + NZ, NZ)
    part_spec = pl.BlockSpec((1, taken, BS), lambda k, me: (k, 0, 0))
    row_spec = pl.BlockSpec((DESTS, MOST, width), lambda k, me: (0, away(k, me), 0))
    in_specs = [
        row_spec,
        pl.BlockSpec((1, BS, width), lambda k, me: (away(k, me), 0, start // width)),
        pl.BlockSpec((1, 1, taken), lambda k, me: (away(k, me), 0, 0)),
    ]
    operands = [rows, table, target]
    if first:
        out_specs = (
            pl.BlockSpec((1, BS + 8, width), lambda k, me: (away(k, me), 0, 0)),
            part_spec,
        )
        out_shape = (
            jax.ShapeDtypeStruct((NZ, BS + 8, width), BF16),
            jax.ShapeDtypeStruct((NZ, taken, BS), F32),
        )
    else:
        in_specs.append(part_spec)
        operands.append(part)
        out_specs = (pl.BlockSpec((BS, width), lambda k, me: (0, 0)),) * NZ + (
            pl.BlockSpec((DESTS, MOST, BS), lambda k, me: (0, away(k, me), 0)),
        )
        out_shape = (jax.ShapeDtypeStruct((BS, width), BF16),) * NZ + (
            jax.ShapeDtypeStruct((DESTS, SLOTS, BS), BF16),
        )
    return pl.pallas_call(
        functools.partial(work_kernel, first),
        grid_spec=pltpu.PrefetchScalarGridSpec(
            num_scalar_prefetch=1,
            grid=(NZ,),
            in_specs=in_specs,
            out_specs=out_specs,
        ),
        out_shape=out_shape,
        cost_estimate=pl.CostEstimate(
            flops=4 * NZ * taken * BS * width,
            bytes_accessed=2 * width * NZ * (taken + 2 * BS) + 8 * NZ * taken * BS,
            transcendentals=0,
        ),
    )(me, *operands)


def return_kernel(slot_ref, returned_ref, out_ref):
    rows = out_ref.shape[0]
    total = returned_ref.shape[0]
    slot = jnp.broadcast_to(slot_ref[...].astype(F32), (128, rows))
    column = jnp.transpose(slot)[:, 0:1].astype(jnp.int32)
    pick = jnp.where(
        lax.broadcasted_iota(jnp.int32, (rows, total), 1) == column, 1.0, 0.0
    ).astype(BF16)
    got = jnp.dot(pick, returned_ref[...], preferred_element_type=F32)
    out_ref[...] = got.astype(BF16)


def pick_back(slot_row, returned):
    npts = slot_row.shape[1]
    rows = 256
    return pl.pallas_call(
        return_kernel,
        grid=(npts // rows,),
        in_specs=[
            pl.BlockSpec((1, rows), lambda i: (0, i)),
            pl.BlockSpec(returned.shape, lambda i: (0, 0)),
        ],
        out_specs=pl.BlockSpec((rows, BS), lambda i: (i, 0)),
        out_shape=jax.ShapeDtypeStruct((npts, BS), BF16),
        cost_estimate=pl.CostEstimate(
            flops=2 * npts * returned.shape[0] * BS,
            bytes_accessed=2 * BS * (npts + returned.shape[0]),
            transcendentals=0,
        ),
    )(slot_row, returned)


def exchange(values, axes):
    return lax.all_to_all(values, axes, split_axis=0, concat_axis=0, tiled=True)


def sum_over_planes(sums):
    total = sums[0].astype(F32)
    for k in sorted(range(1, NZ), key=lambda k: -min(k, NZ - k)):
        got = lax.ppermute(sums[k], "z", [(i, (i - k) % NZ) for i in range(NZ)])
        total = total + got.astype(F32)
    return total


def shards(points, blocks, finals, centroids):
    npts, _ = points.shape
    group = lax.axis_index("x") * NC + lax.axis_index("c")
    me = lax.axis_index("z").astype(jnp.int32).reshape(1)
    own = lax.dynamic_slice_in_dim(centroids, group * BS, BS, 0)
    table = lax.all_gather(own, "z", axis=0, tiled=False)

    block_row = blocks.reshape(1, npts)
    final_row = finals.reshape(1, npts)
    cut = WIDTHS[0]
    sent, slot_row = prepare(block_row, final_row, points, 0, cut, None)
    here = exchange(sent, PLANE)
    sent = prepare(block_row, final_row, points, cut, WIDTHS[1], slot_row)
    then = exchange(sent, PLANE)
    target = here[:, SLOTS, :SLOTS].astype(jnp.int32) - 1
    target = jnp.transpose(target.reshape(DESTS, NZ, MOST), (1, 0, 2))
    target = target.reshape(NZ, 1, DESTS * MOST)
    sums, part = block_work(me, here, table, target, None, 0)
    share = lax.psum_scatter(sums, "z", scatter_dimension=0, tiled=True)[0]
    *rest, part = block_work(me, then, table, target, part, cut)
    returned = exchange(part, PLANE).reshape(DESTS * SLOTS, BS)
    rest = sum_over_planes(rest)
    distances = pick_back(slot_row, returned)

    counts = share[BS, :BS].astype(F32) + 16.0 * share[BS + 1, :BS].astype(F32)
    total = jnp.concatenate([share[:BS].astype(F32), rest], axis=1)
    fresh = (total + own.astype(F32)) / (counts + 1.0)[:, None]
    fresh = lax.all_to_all(
        fresh.astype(BF16), ("x", "c"), split_axis=1, concat_axis=0, tiled=True
    )
    return distances, fresh.astype(F32)


def solution(mesh):
    split = Mesh(mesh.devices.reshape(NX, NC, NZ, NY), ("x", "c", "z", "y"))
    every = ("x", "c", "z", "y")
    placed = (P(every, None), P(every, None), P(every), P(("z", "y"), None))
    return jax.shard_map(
        shards,
        mesh=split,
        in_specs=placed,
        out_specs=(P(every, None), P(("z", "y"), ("x", "c"))),
        check_vma=False,
    )
```

```python
import functools

import jax
import jax.numpy as jnp
from jax import lax
from jax.experimental import pallas as pl
from jax.experimental.pallas import tpu as pltpu
from jax.sharding import Mesh
from jax.sharding import PartitionSpec as P

BS = 256
MOST = 16
NX, NC, NZ, NY = 4, 2, 8, 4
NG = NX * NC
NB = NZ * NY * NG
DESTS = NG * NY
SLOTS = NZ * MOST
WIDTHS = (384, 384, 256)
PLANE = ("x", "c", "y")
DIGIT = 64
GRANT = 32 * 2**20
PAIR = 2
PER_STEP = 4
F32, BF16 = jnp.float32, jnp.bfloat16


def mask(where):
    return jnp.where(where, jnp.ones((), BF16), jnp.zeros((), BF16))


def nt_dot(a, b):
    return lax.dot_general(a, b, (((1,), (1,)), ((), ())), preferred_element_type=F32)


def slots_of(block_row):
    npts = block_row.shape[1]
    piece = 128
    row = lax.broadcasted_iota(jnp.int32, (piece, 2 * piece), 0)
    column = lax.broadcasted_iota(jnp.int32, (piece, 2 * piece), 1)
    before = jnp.where((row < column) | (column >= piece), 1.0, 0.0).astype(BF16)
    carry = jnp.zeros((NB, piece), F32)
    ranks = []
    for i in range(npts // piece):
        part = block_row[:, i * piece : (i + 1) * piece]
        member = lax.broadcasted_iota(jnp.int32, (NB, piece), 0) == part
        ones = jnp.where(member, 1.0, 0.0)
        seen = jnp.dot(ones.astype(BF16), before, preferred_element_type=F32)
        ranks.append(jnp.sum(ones * (seen[:, :piece] + carry), axis=0, keepdims=True))
        carry = carry + seen[:, piece:]
    rank = jnp.concatenate(ranks, axis=1).astype(jnp.int32)
    zz = block_row // (NY * NG)
    yy = (block_row // NG) % NY
    gg = block_row % NG
    return ((gg * NY + yy) * NZ + zz) * MOST + rank


def low_digits(slots):
    line = lax.broadcasted_iota(jnp.int32, (DIGIT, slots.shape[1]), 0)
    return jnp.where(line == slots % DIGIT, 1.0, 0.0).astype(BF16)


def pick_rows(slots, low, base, rows):
    npts = slots.shape[1]
    line = lax.broadcasted_iota(jnp.int32, (rows // DIGIT, npts), 0)
    high = jnp.where(line + base // DIGIT == slots // DIGIT, 1.0, 0.0)
    parts = []
    for i in range(rows // DIGIT):
        one = jnp.broadcast_to(high[i : i + 1], (16, npts)).astype(BF16)
        parts.append(low * jnp.concatenate([one] * (DIGIT // 16), axis=0))
    return jnp.concatenate(parts, axis=0)


def first_prep(block_ref, final_ref, points_ref, out_ref, slot_ref, slots, low, targets):
    step = pl.program_id(0)

    @pl.when(step == 0)
    def _():
        found = slots_of(block_ref[...])
        slots[...] = found
        slot_ref[...] = found
        low[...] = low_digits(found)
        line = lax.broadcasted_iota(jnp.int32, (DESTS * SLOTS // DIGIT, found.shape[1]), 0)
        high = jnp.where(line == found // DIGIT, (final_ref[...] + 1).astype(F32), 0.0)
        targets[...] = nt_dot(high.astype(BF16), low[...])

    rows = PER_STEP * SLOTS
    width = points_ref.shape[1]
    pick = pick_rows(slots[...], low[...], step * rows, rows)
    moved = jnp.dot(pick, points_ref[...], preferred_element_type=F32)
    out_ref[:, 0:SLOTS] = moved.astype(BF16).reshape(PER_STEP, SLOTS, width)
    digits = rows // DIGIT
    target = targets[pl.ds(pl.multiple_of(step * digits, digits), digits)]
    blank = jnp.zeros((1, width - SLOTS), F32)
    for i in range(PER_STEP):
        each = SLOTS // DIGIT
        one = [target[j : j + 1] for j in range(i * each, (i + 1) * each)]
        one = jnp.concatenate(one + [blank], axis=1)
        out_ref[i, SLOTS : SLOTS + 8] = jnp.broadcast_to(one, (8, width)).astype(BF16)


def later_prep(slot_ref, points_ref, out_ref, low):
    step = pl.program_id(0)

    @pl.when(step == 0)
    def _():
        low[...] = low_digits(slot_ref[...])

    rows = PER_STEP * SLOTS
    pick = pick_rows(slot_ref[...], low[...], step * rows, rows)
    moved = jnp.dot(pick, points_ref[...], preferred_element_type=F32)
    out_ref[...] = moved.astype(BF16).reshape(out_ref.shape)


def prepare(block_row, final_row, points, start, width, slot_row):
    npts = points.shape[0]
    steps = DESTS // PER_STEP
    column = start // width
    whole = pl.BlockSpec((1, npts), lambda i: (0, 0))
    point_spec = pl.BlockSpec((npts, width), lambda i: (0, column))
    tall = SLOTS if slot_row is not None else SLOTS + 8
    out_spec = pl.BlockSpec((PER_STEP, tall, width), lambda i: (i, 0, 0))
    out_shape = jax.ShapeDtypeStruct((DESTS, tall, width), BF16)
    cost = pl.CostEstimate(
        flops=2 * DESTS * SLOTS * npts * width,
        bytes_accessed=2 * width * (npts + DESTS * SLOTS),
        transcendentals=0,
    )
    if slot_row is not None:
        return pl.pallas_call(
            later_prep,
            grid=(steps,),
            in_specs=[whole, point_spec],
            out_specs=out_spec,
            out_shape=out_shape,
            scratch_shapes=[pltpu.VMEM((DIGIT, npts), BF16)],
            cost_estimate=cost,
        )(slot_row, points)
    return pl.pallas_call(
        first_prep,
        grid=(steps,),
        in_specs=[whole, whole, point_spec],
        out_specs=(out_spec, whole),
        out_shape=(out_shape, jax.ShapeDtypeStruct((1, npts), jnp.int32)),
        scratch_shapes=[
            pltpu.VMEM((1, npts), jnp.int32),
            pltpu.VMEM((DIGIT, npts), BF16),
            pltpu.VMEM((DESTS * SLOTS // DIGIT, DIGIT), F32),
        ],
        cost_estimate=cost,
    )(block_row, final_row, points)


def work_kernel(first, last, me_ref, *refs):
    refs = list(refs)
    rows_ref, target_ref = refs[:2]
    piece_refs = refs[2 : 2 + NZ]
    part_ref = None if first else refs[2 + NZ]
    sum_refs, result_ref, tables, packs = refs[-NZ - 3 : -3], refs[-3], refs[-2], refs[-1]
    places = [
        lax.rem(me_ref[0] - (pl.program_id(0) * PAIR + b) + NZ, NZ) for b in range(PAIR)
    ]
    for b in range(PAIR):
        for i in range(NZ):

            @pl.when(places[b] == i)
            def _(b=b, i=i):
                tables[b] = piece_refs[i][...]

    for b in range(PAIR):
        rows = rows_ref[:, b * MOST : (b + 1) * MOST, :].reshape(DESTS * MOST, rows_ref.shape[-1])
        table = tables[b]
        onehot = jnp.where(
            lax.broadcasted_iota(jnp.int32, (BS, DESTS * MOST), 0) == target_ref[b], 1.0, 0.0
        ).astype(BF16)
        sums = jnp.dot(onehot, rows, preferred_element_type=F32)
        packs[b, 0:BS] = sums.astype(BF16)
        if first:
            ones = jnp.ones((8, DESTS * MOST), BF16)
            count = nt_dot(ones, onehot)
            high = jnp.floor(count * (1.0 / 16.0))
            low = count - 16.0 * high
            which = lax.broadcasted_iota(jnp.int32, count.shape, 0)
            digits = jnp.where(which == 0, low, jnp.where(which == 1, high, 0.0))
            blank = jnp.zeros((8, sums.shape[1] - BS), F32)
            packs[b, BS : BS + 8] = jnp.concatenate([digits, blank], axis=1).astype(BF16)
        cross = nt_dot(rows, table)
        wide = rows.astype(F32)
        row_norm = jnp.sum(wide * wide, axis=1, keepdims=True)
        tall = table.astype(F32)
        cent_norm = jnp.sum(tall * tall, axis=1, keepdims=True)
        cent_norm = jnp.transpose(jnp.broadcast_to(cent_norm, (BS, 128)))[0:1]
        total = row_norm - 2.0 * cross + cent_norm
        if not first:
            total = total + part_ref[b]
        if last:
            total = (total * (1.0 / 1024.0)).astype(BF16)
            result_ref[:, b * MOST : (b + 1) * MOST, :] = total.reshape(DESTS, MOST, BS)
        else:
            result_ref[b] = total
    for b in range(PAIR):
        for i in range(NZ):

            @pl.when(places[b] == i)
            def _(b=b, i=i):
                sum_refs[i][...] = packs[b]


def block_work(me, rows, pieces, target, part, start, last):
    width = rows.shape[-1]
    first = part is None
    taken = DESTS * MOST
    tall = BS + 8 if first else BS
    row_spec = pl.BlockSpec((DESTS, PAIR * MOST, width), lambda k, me: (0, k, 0))
    part_spec = pl.BlockSpec((PAIR, taken, BS), lambda k, me: (k, 0, 0))
    in_specs = [row_spec, pl.BlockSpec((PAIR, 1, taken), lambda k, me: (k, 0, 0))]
    in_specs += [pl.BlockSpec((BS, width), lambda k, me: (0, start // width))] * NZ
    operands = [rows, target, *pieces]
    if not first:
        in_specs.append(part_spec)
        operands.append(part)
    if last:
        result_spec = pl.BlockSpec((DESTS, PAIR * MOST, BS), lambda k, me: (0, k, 0))
        result_shape = jax.ShapeDtypeStruct((DESTS, SLOTS, BS), BF16)
    else:
        result_spec = part_spec
        result_shape = jax.ShapeDtypeStruct((NZ, taken, BS), F32)
    return pl.pallas_call(
        functools.partial(work_kernel, first, last),
        grid_spec=pltpu.PrefetchScalarGridSpec(
            num_scalar_prefetch=1,
            grid=(NZ // PAIR,),
            in_specs=in_specs,
            out_specs=(pl.BlockSpec((tall, width), lambda k, me: (0, 0)),) * NZ + (result_spec,),
            scratch_shapes=[
                pltpu.VMEM((PAIR, BS, width), BF16),
                pltpu.VMEM((PAIR, tall, width), BF16),
            ],
        ),
        out_shape=(jax.ShapeDtypeStruct((tall, width), BF16),) * NZ + (result_shape,),
        cost_estimate=pl.CostEstimate(
            flops=4 * NZ * taken * BS * width,
            bytes_accessed=2 * width * NZ * (taken + 2 * BS) + 8 * NZ * taken * BS,
            transcendentals=0,
        ),
    )(me, *operands)


def return_kernel(slot_ref, returned_ref, out_ref):
    rows = out_ref.shape[0]
    lane = 128
    slot = jnp.transpose(jnp.broadcast_to(slot_ref[...].astype(F32), (lane, rows)))
    slot = slot.astype(jnp.int32)
    hit = slot % lane == lax.broadcasted_iota(jnp.int32, (rows, lane), 1)
    high = jnp.where(hit, slot // lane, -1).astype(F32).astype(BF16)
    total = jnp.zeros(out_ref.shape, F32)
    part = 1024
    for at in range(0, returned_ref.shape[0], part):
        pick = [mask(high == jnp.asarray(i // lane, BF16)) for i in range(at, at + part, lane)]
        pick = jnp.concatenate(pick, axis=1)
        total += jnp.dot(pick, returned_ref[at : at + part], preferred_element_type=F32)
    out_ref[...] = total.astype(BF16)


def pick_back(slot_row, returned):
    npts = slot_row.shape[1]
    rows = 512
    return pl.pallas_call(
        return_kernel,
        grid=(npts // rows,),
        in_specs=[
            pl.BlockSpec((1, rows), lambda i: (0, i)),
            pl.BlockSpec(returned.shape, lambda i: (0, 0)),
        ],
        out_specs=pl.BlockSpec((rows, BS), lambda i: (i, 0)),
        out_shape=jax.ShapeDtypeStruct((npts, BS), BF16),
        compiler_params=pltpu.CompilerParams(vmem_limit_bytes=GRANT),
        cost_estimate=pl.CostEstimate(
            flops=2 * npts * returned.shape[0] * BS,
            bytes_accessed=2 * BS * (npts + returned.shape[0]),
            transcendentals=0,
        ),
    )(slot_row, returned)


def exchange(values, axes):
    return lax.all_to_all(values, axes, split_axis=0, concat_axis=0, tiled=True)


def pass_on(values, distance):
    return lax.ppermute(values, "z", [(i, (i + distance) % NZ) for i in range(NZ)])


def gather_table(own):
    up, down, below, above = own, own, [], []
    for step in range(1, NZ // 2 + 1):
        up = pass_on(up, 1)
        below.append(up)
        if step < NZ // 2:
            down = pass_on(down, -1)
            above.append(down)
    return [own, *below, *reversed(above)]


def sum_over_planes(sums):
    total = sums[0].astype(F32)
    for k in sorted(range(1, NZ), key=lambda k: -min(k, NZ - k)):
        total = total + pass_on(sums[k], -k).astype(F32)
    return total


def shards(points, blocks, finals, centroids):
    npts, _ = points.shape
    group = lax.axis_index("x") * NC + lax.axis_index("c")
    me = lax.axis_index("z").astype(jnp.int32).reshape(1)
    own = lax.dynamic_slice_in_dim(centroids, group * BS, BS, 0)
    pieces = gather_table(own)

    block_row = blocks.reshape(1, npts)
    final_row = finals.reshape(1, npts)
    last = len(WIDTHS) - 1
    starts = [sum(WIDTHS[:i]) for i in range(last + 1)]
    arrived, slot_row = [], None
    for i, size in enumerate(WIDTHS):
        sent = prepare(block_row, final_row, points, starts[i], size, slot_row)
        if i == 0:
            sent, slot_row = sent
        arrived.append(exchange(sent, PLANE))
    target = arrived[0][:, SLOTS, :SLOTS].astype(jnp.int32) - 1
    target = jnp.transpose(target.reshape(DESTS, NZ, MOST), (1, 0, 2))
    target = target.reshape(NZ, 1, DESTS * MOST)
    part, shares = None, []
    for i in range(last + 1):
        *sums, part = block_work(
            me, arrived[i], pieces, target, part, starts[i], i == last
        )
        shares.append(sum_over_planes(sums))
    returned = exchange(part, PLANE).reshape(DESTS * SLOTS, BS)
    distances = pick_back(slot_row, returned)

    counts = shares[0][BS, :BS] + 16.0 * shares[0][BS + 1, :BS]
    total = jnp.concatenate([s[:BS] for s in shares], axis=1)
    fresh = (total + own.astype(F32)) / (counts + 1.0)[:, None]
    fresh = lax.all_to_all(fresh.astype(BF16), ("x", "c"), split_axis=1, concat_axis=0, tiled=True)
    return distances, fresh.astype(F32)


def solution(mesh):
    split = Mesh(mesh.devices.reshape(NX, NC, NZ, NY), ("x", "c", "z", "y"))
    every = ("x", "c", "z", "y")
    placed = (P(every, None), P(every, None), P(every), P(("z", "y"), None))
    return jax.shard_map(
        shards,
        mesh=split,
        in_specs=placed,
        out_specs=(P(every, None), P(("z", "y"), ("x", "c"))),
        check_vma=False,
    )
```

```python
import functools

import jax
import jax.numpy as jnp
from jax import lax
from jax.experimental import pallas as pl
from jax.experimental.pallas import tpu as pltpu
from jax.sharding import Mesh
from jax.sharding import PartitionSpec as P

BS = 256
MOST = 16
NX, NC, NZ, NY = 4, 2, 8, 4
NG = NX * NC
NB = NZ * NY * NG
DESTS = NG * NY
SLOTS = NZ * MOST
WIDTHS = (512, 256, 256)
PLANE = ("x", "c", "y")
DIGIT = 64
GRANT = 32 * 2**20
WHOLE = 67043328
PAIR = 2
PER_STEP = 4
F32, BF16 = jnp.float32, jnp.bfloat16


def mask(where):
    return jnp.where(where, jnp.ones((), BF16), jnp.zeros((), BF16))


def nt_dot(a, b):
    return lax.dot_general(a, b, (((1,), (1,)), ((), ())), preferred_element_type=F32)


def slots_of(block_row):
    npts = block_row.shape[1]
    piece = 128
    row = lax.broadcasted_iota(jnp.int32, (piece, 2 * piece), 0)
    column = lax.broadcasted_iota(jnp.int32, (piece, 2 * piece), 1)
    before = jnp.where((row < column) | (column >= piece), 1.0, 0.0).astype(BF16)
    carry = jnp.zeros((NB, piece), F32)
    ranks = []
    for i in range(npts // piece):
        part = block_row[:, i * piece : (i + 1) * piece]
        member = lax.broadcasted_iota(jnp.int32, (NB, piece), 0) == part
        ones = jnp.where(member, 1.0, 0.0)
        seen = jnp.dot(ones.astype(BF16), before, preferred_element_type=F32)
        ranks.append(jnp.sum(ones * (seen[:, :piece] + carry), axis=0, keepdims=True))
        carry = carry + seen[:, piece:]
    rank = jnp.concatenate(ranks, axis=1).astype(jnp.int32)
    zz = block_row // (NY * NG)
    yy = (block_row // NG) % NY
    gg = block_row % NG
    return ((gg * NY + yy) * NZ + zz) * MOST + rank


def low_digits(slots):
    line = lax.broadcasted_iota(jnp.int32, (DIGIT, slots.shape[1]), 0)
    return jnp.where(line == slots % DIGIT, 1.0, 0.0).astype(BF16)


def pick_rows(slots, low, base, rows):
    npts = slots.shape[1]
    line = lax.broadcasted_iota(jnp.int32, (rows // DIGIT, npts), 0)
    high = jnp.where(line + base // DIGIT == slots // DIGIT, 1.0, 0.0)
    parts = []
    for i in range(rows // DIGIT):
        one = jnp.broadcast_to(high[i : i + 1], (16, npts)).astype(BF16)
        parts.append(low * jnp.concatenate([one] * (DIGIT // 16), axis=0))
    return jnp.concatenate(parts, axis=0)


def first_prep(block_ref, final_ref, points_ref, out_ref, slot_ref, slots, low, targets):
    step = pl.program_id(0)

    @pl.when(step == 0)
    def _():
        found = slots_of(block_ref[...])
        slots[...] = found
        slot_ref[...] = found
        low[...] = low_digits(found)
        line = lax.broadcasted_iota(jnp.int32, (DESTS * SLOTS // DIGIT, found.shape[1]), 0)
        high = jnp.where(line == found // DIGIT, (final_ref[...] + 1).astype(F32), 0.0)
        targets[...] = nt_dot(high.astype(BF16), low[...])

    rows = PER_STEP * SLOTS
    width = points_ref.shape[1]
    pick = pick_rows(slots[...], low[...], step * rows, rows)
    moved = jnp.dot(pick, points_ref[...], preferred_element_type=F32)
    out_ref[:, 0:SLOTS] = moved.astype(BF16).reshape(PER_STEP, SLOTS, width)
    digits = rows // DIGIT
    target = targets[pl.ds(pl.multiple_of(step * digits, digits), digits)]
    blank = jnp.zeros((1, width - SLOTS), F32)
    for i in range(PER_STEP):
        each = SLOTS // DIGIT
        one = [target[j : j + 1] for j in range(i * each, (i + 1) * each)]
        one = jnp.concatenate(one + [blank], axis=1)
        out_ref[i, SLOTS : SLOTS + 8] = jnp.broadcast_to(one, (8, width)).astype(BF16)


def later_prep(slot_ref, points_ref, out_ref, low):
    step = pl.program_id(0)

    @pl.when(step == 0)
    def _():
        low[...] = low_digits(slot_ref[...])

    rows = PER_STEP * SLOTS
    pick = pick_rows(slot_ref[...], low[...], step * rows, rows)
    moved = jnp.dot(pick, points_ref[...], preferred_element_type=F32)
    out_ref[...] = moved.astype(BF16).reshape(out_ref.shape)


def prepare(block_row, final_row, points, start, width, slot_row):
    npts = points.shape[0]
    steps = DESTS // PER_STEP
    column = start // width
    whole = pl.BlockSpec((1, npts), lambda i: (0, 0))
    point_spec = pl.BlockSpec((npts, width), lambda i: (0, column))
    tall = SLOTS if slot_row is not None else SLOTS + 8
    out_spec = pl.BlockSpec((PER_STEP, tall, width), lambda i: (i, 0, 0))
    out_shape = jax.ShapeDtypeStruct((DESTS, tall, width), BF16)
    cost = pl.CostEstimate(
        flops=2 * DESTS * SLOTS * npts * width,
        bytes_accessed=2 * width * (npts + DESTS * SLOTS),
        transcendentals=0,
    )
    if slot_row is not None:
        return pl.pallas_call(
            later_prep,
            grid=(steps,),
            in_specs=[whole, point_spec],
            out_specs=out_spec,
            out_shape=out_shape,
            scratch_shapes=[pltpu.VMEM((DIGIT, npts), BF16)],
            cost_estimate=cost,
        )(slot_row, points)
    return pl.pallas_call(
        first_prep,
        grid=(steps,),
        in_specs=[whole, whole, point_spec],
        out_specs=(out_spec, whole),
        out_shape=(out_shape, jax.ShapeDtypeStruct((1, npts), jnp.int32)),
        scratch_shapes=[
            pltpu.VMEM((1, npts), jnp.int32),
            pltpu.VMEM((DIGIT, npts), BF16),
            pltpu.VMEM((DESTS * SLOTS // DIGIT, DIGIT), F32),
        ],
        cost_estimate=cost,
    )(block_row, final_row, points)


def block_rows(rows_ref, b):
    rows = rows_ref[:, b * MOST : (b + 1) * MOST, :]
    return rows.reshape(DESTS * MOST, rows_ref.shape[-1])


def places_of(me_ref):
    base = me_ref[0] + NZ - pl.program_id(0) * PAIR
    return [lax.rem(base - b, NZ) for b in range(PAIR)]


def sums_kernel(first, me_ref, rows_ref, target_ref, *refs):
    sum_refs, packs = refs[:NZ], refs[NZ]
    for b in range(PAIR):
        rows = block_rows(rows_ref, b)
        onehot = jnp.where(
            lax.broadcasted_iota(jnp.int32, (BS, DESTS * MOST), 0) == target_ref[b], 1.0, 0.0
        ).astype(BF16)
        sums = jnp.dot(onehot, rows, preferred_element_type=F32)
        packs[b, 0:BS] = sums.astype(BF16)
        if first:
            ones = jnp.ones((8, DESTS * MOST), BF16)
            count = nt_dot(ones, onehot)
            high = jnp.floor(count * (1.0 / 16.0))
            low = count - 16.0 * high
            which = lax.broadcasted_iota(jnp.int32, count.shape, 0)
            digits = jnp.where(which == 0, low, jnp.where(which == 1, high, 0.0))
            blank = jnp.zeros((8, sums.shape[1] - BS), F32)
            packs[b, BS : BS + 8] = jnp.concatenate([digits, blank], axis=1).astype(BF16)
    for b, place in enumerate(places_of(me_ref)):
        for i in range(NZ):

            @pl.when(place == i)
            def _(b=b, i=i):
                sum_refs[i][...] = packs[b]


def distance_kernel(first, last, me_ref, rows_ref, *refs):
    piece_refs = refs[:NZ]
    part_ref = None if first else refs[NZ]
    result_ref, tables = refs[-2], refs[-1]
    for b, place in enumerate(places_of(me_ref)):
        for i in range(NZ):

            @pl.when(place == i)
            def _(b=b, i=i):
                tables[b] = piece_refs[i][...]

    for b in range(PAIR):
        rows = block_rows(rows_ref, b)
        table = tables[b]
        cross = nt_dot(rows, table)
        wide = rows.astype(F32)
        row_norm = jnp.sum(wide * wide, axis=1, keepdims=True)
        tall = table.astype(F32)
        cent_norm = jnp.sum(tall * tall, axis=1, keepdims=True)
        cent_norm = jnp.transpose(jnp.broadcast_to(cent_norm, (BS, 128)))[0:1]
        total = row_norm - 2.0 * cross + cent_norm
        if not first:
            total = total + part_ref[b]
        if last:
            total = (total * (1.0 / 1024.0)).astype(BF16)
            result_ref[:, b * MOST : (b + 1) * MOST, :] = total.reshape(DESTS, MOST, BS)
        else:
            result_ref[b] = total


def both_kernel(first, me_ref, rows_ref, target_ref, *refs):
    inputs = refs[: NZ if first else NZ + 1]
    outputs = refs[len(inputs) :]
    sum_refs, result_ref, packs, tables = outputs[:NZ], outputs[NZ], outputs[-2], outputs[-1]
    distance_kernel(first, False, me_ref, rows_ref, *inputs, result_ref, tables)
    sums_kernel(first, me_ref, rows_ref, target_ref, *sum_refs, packs)


def block_work(me, rows, pieces, target, part, start, kind):
    width = rows.shape[-1]
    first, last = part is None, kind == "distances"
    taken = DESTS * MOST
    tall = BS + 8 if first and kind == "both" else BS
    row_spec = pl.BlockSpec((DESTS, PAIR * MOST, width), lambda k, me: (0, k, 0))
    part_spec = pl.BlockSpec((PAIR, taken, BS), lambda k, me: (k, 0, 0))
    operands, in_specs = [rows], [row_spec]
    out_shape, out_specs, scratch = [], [], []
    if kind != "distances":
        operands.append(target)
        in_specs.append(pl.BlockSpec((PAIR, 1, taken), lambda k, me: (k, 0, 0)))
        out_shape += [jax.ShapeDtypeStruct((tall, width), BF16)] * NZ
        out_specs += [pl.BlockSpec((tall, width), lambda k, me: (0, 0))] * NZ
        scratch.append(pltpu.VMEM((PAIR, tall, width), BF16))
    if kind != "sums":
        operands += pieces
        in_specs += [pl.BlockSpec((BS, width), lambda k, me: (0, start // width))] * NZ
        scratch.append(pltpu.VMEM((PAIR, BS, width), BF16))
        if not first:
            operands.append(part)
            in_specs.append(part_spec)
        if last:
            out_shape.append(jax.ShapeDtypeStruct((DESTS, SLOTS, BS), BF16))
            out_specs.append(pl.BlockSpec((DESTS, PAIR * MOST, BS), lambda k, me: (0, k, 0)))
        else:
            out_shape.append(jax.ShapeDtypeStruct((NZ, taken, BS), F32))
            out_specs.append(part_spec)
    kernel = {
        "both": functools.partial(both_kernel, first),
        "sums": functools.partial(sums_kernel, False),
        "distances": functools.partial(distance_kernel, first, True),
    }[kind]
    return pl.pallas_call(
        kernel,
        grid_spec=pltpu.PrefetchScalarGridSpec(
            num_scalar_prefetch=1,
            grid=(NZ // PAIR,),
            in_specs=in_specs,
            out_specs=out_specs,
            scratch_shapes=scratch,
        ),
        out_shape=out_shape,
        compiler_params=pltpu.CompilerParams(
            vmem_limit_bytes=WHOLE if kind == "both" else None
        ),
        cost_estimate=pl.CostEstimate(
            flops=4 * NZ * taken * BS * width,
            bytes_accessed=2 * width * NZ * (taken + 2 * BS) + 8 * NZ * taken * BS,
            transcendentals=0,
        ),
    )(me, *operands)


def return_kernel(slot_ref, returned_ref, out_ref):
    rows = out_ref.shape[0]
    lane = 128
    slot = jnp.transpose(jnp.broadcast_to(slot_ref[...].astype(F32), (lane, rows)))
    slot = slot.astype(jnp.int32)
    hit = slot % lane == lax.broadcasted_iota(jnp.int32, (rows, lane), 1)
    high = jnp.where(hit, slot // lane, -1).astype(F32).astype(BF16)
    total = jnp.zeros(out_ref.shape, F32)
    part = 1024
    for at in range(0, returned_ref.shape[0], part):
        pick = [mask(high == jnp.asarray(i // lane, BF16)) for i in range(at, at + part, lane)]
        pick = jnp.concatenate(pick, axis=1)
        total += jnp.dot(pick, returned_ref[at : at + part], preferred_element_type=F32)
    out_ref[...] = total.astype(BF16)


def pick_back(slot_row, returned):
    npts = slot_row.shape[1]
    rows = 512
    return pl.pallas_call(
        return_kernel,
        grid=(npts // rows,),
        in_specs=[
            pl.BlockSpec((1, rows), lambda i: (0, i)),
            pl.BlockSpec(returned.shape, lambda i: (0, 0)),
        ],
        out_specs=pl.BlockSpec((rows, BS), lambda i: (i, 0)),
        out_shape=jax.ShapeDtypeStruct((npts, BS), BF16),
        compiler_params=pltpu.CompilerParams(vmem_limit_bytes=GRANT),
        cost_estimate=pl.CostEstimate(
            flops=2 * npts * returned.shape[0] * BS,
            bytes_accessed=2 * BS * (npts + returned.shape[0]),
            transcendentals=0,
        ),
    )(slot_row, returned)


def exchange(values, axes):
    return lax.all_to_all(values, axes, split_axis=0, concat_axis=0, tiled=True)


def pass_on(values, distance):
    return lax.ppermute(values, "z", [(i, (i + distance) % NZ) for i in range(NZ)])


def gather_table(own):
    up, down, below, above = own, own, [], []
    for step in range(1, NZ // 2 + 1):
        up = pass_on(up, 1)
        below.append(up)
        if step < NZ // 2:
            down = pass_on(down, -1)
            above.append(down)
    return [own, *below, *reversed(above)]


def sum_over_planes(sums):
    total = sums[0].astype(F32)
    for k in sorted(range(1, NZ), key=lambda k: -min(k, NZ - k)):
        total = total + pass_on(sums[k], -k).astype(F32)
    return total


def shards(points, blocks, finals, centroids):
    npts, _ = points.shape
    group = lax.axis_index("x") * NC + lax.axis_index("c")
    me = lax.axis_index("z").astype(jnp.int32).reshape(1)
    own = lax.dynamic_slice_in_dim(centroids, group * BS, BS, 0)
    pieces = gather_table(own)

    block_row = blocks.reshape(1, npts)
    final_row = finals.reshape(1, npts)
    last = len(WIDTHS) - 1
    starts = [sum(WIDTHS[:i]) for i in range(last + 1)]
    arrived, slot_row = [], None
    for i, size in enumerate(WIDTHS):
        sent = prepare(block_row, final_row, points, starts[i], size, slot_row)
        if i == 0:
            sent, slot_row = sent
        arrived.append(exchange(sent, PLANE))
    target = arrived[0][:, SLOTS, :SLOTS].astype(jnp.int32) - 1
    target = jnp.transpose(target.reshape(DESTS, NZ, MOST), (1, 0, 2))
    target = target.reshape(NZ, 1, DESTS * MOST)
    part, shares = None, []
    for i in range(last):
        *sums, part = block_work(me, arrived[i], pieces, target, part, starts[i], "both")
        shares.append(sum_over_planes(sums))
    (part,) = block_work(
        me, arrived[last], pieces, target, part, starts[last], "distances"
    )
    returned = exchange(part, PLANE).reshape(DESTS * SLOTS, BS)
    sums = block_work(me, arrived[last], pieces, target, part, starts[last], "sums")
    shares.append(sum_over_planes(sums))
    distances = pick_back(slot_row, returned)

    counts = shares[0][BS, :BS] + 16.0 * shares[0][BS + 1, :BS]
    total = jnp.concatenate([s[:BS] for s in shares], axis=1)
    fresh = (total + own.astype(F32)) / (counts + 1.0)[:, None]
    fresh = lax.all_to_all(fresh.astype(BF16), ("x", "c"), split_axis=1, concat_axis=0, tiled=True)
    return distances, fresh.astype(F32)


def solution(mesh):
    split = Mesh(mesh.devices.reshape(NX, NC, NZ, NY), ("x", "c", "z", "y"))
    every = ("x", "c", "z", "y")
    placed = (P(every, None), P(every, None), P(every), P(("z", "y"), None))
    return jax.shard_map(
        shards,
        mesh=split,
        in_specs=placed,
        out_specs=(P(every, None), P(("z", "y"), ("x", "c"))),
        check_vma=False,
    )
```

```python
import functools

import jax
import jax.numpy as jnp
from jax import lax
from jax.experimental import pallas as pl
from jax.experimental.pallas import tpu as pltpu
from jax.sharding import Mesh
from jax.sharding import PartitionSpec as P

BS = 256
MOST = 16
NX, NC, NZ, NY = 4, 2, 8, 4
NG = NX * NC
NB = NZ * NY * NG
DESTS = NG * NY
SLOTS = NZ * MOST
WIDTHS = (384, 384, 256)
PLANE = ("x", "c", "y")
DIGIT = 64
GRANT = 32 * 2**20
WHOLE = 67043328
PAIR = 2
PER_STEP = 4
F32, BF16 = jnp.float32, jnp.bfloat16


def mask(where):
    return jnp.where(where, jnp.ones((), BF16), jnp.zeros((), BF16))


def nt_dot(a, b):
    return lax.dot_general(a, b, (((1,), (1,)), ((), ())), preferred_element_type=F32)


def slots_of(block_row):
    npts = block_row.shape[1]
    piece = 128
    row = lax.broadcasted_iota(jnp.int32, (piece, 2 * piece), 0)
    column = lax.broadcasted_iota(jnp.int32, (piece, 2 * piece), 1)
    before = jnp.where((row < column) | (column >= piece), 1.0, 0.0).astype(BF16)
    carry = jnp.zeros((NB, piece), F32)
    ranks = []
    for i in range(npts // piece):
        part = block_row[:, i * piece : (i + 1) * piece]
        member = lax.broadcasted_iota(jnp.int32, (NB, piece), 0) == part
        ones = jnp.where(member, 1.0, 0.0)
        seen = jnp.dot(ones.astype(BF16), before, preferred_element_type=F32)
        ranks.append(jnp.sum(ones * (seen[:, :piece] + carry), axis=0, keepdims=True))
        carry = carry + seen[:, piece:]
    rank = jnp.concatenate(ranks, axis=1).astype(jnp.int32)
    zz = block_row // (NY * NG)
    yy = (block_row // NG) % NY
    gg = block_row % NG
    return ((gg * NY + yy) * NZ + zz) * MOST + rank


def low_digits(slots):
    line = lax.broadcasted_iota(jnp.int32, (DIGIT, slots.shape[1]), 0)
    return jnp.where(line == slots % DIGIT, 1.0, 0.0).astype(BF16)


def pick_rows(slots, low, base, rows):
    npts = slots.shape[1]
    line = lax.broadcasted_iota(jnp.int32, (rows // DIGIT, npts), 0)
    high = jnp.where(line + base // DIGIT == slots // DIGIT, 1.0, 0.0)
    parts = []
    for i in range(rows // DIGIT):
        one = jnp.broadcast_to(high[i : i + 1], (16, npts)).astype(BF16)
        parts.append(low * jnp.concatenate([one] * (DIGIT // 16), axis=0))
    return jnp.concatenate(parts, axis=0)


def first_prep(block_ref, final_ref, points_ref, out_ref, slot_ref, slots, low, targets):
    step = pl.program_id(0)

    @pl.when(step == 0)
    def _():
        found = slots_of(block_ref[...])
        slots[...] = found
        slot_ref[...] = found
        low[...] = low_digits(found)
        line = lax.broadcasted_iota(jnp.int32, (DESTS * SLOTS // DIGIT, found.shape[1]), 0)
        high = jnp.where(line == found // DIGIT, (final_ref[...] + 1).astype(F32), 0.0)
        targets[...] = nt_dot(high.astype(BF16), low[...])

    rows = PER_STEP * SLOTS
    width = points_ref.shape[1]
    pick = pick_rows(slots[...], low[...], step * rows, rows)
    moved = jnp.dot(pick, points_ref[...], preferred_element_type=F32)
    out_ref[:, 0:SLOTS] = moved.astype(BF16).reshape(PER_STEP, SLOTS, width)
    digits = rows // DIGIT
    target = targets[pl.ds(pl.multiple_of(step * digits, digits), digits)]
    blank = jnp.zeros((1, width - SLOTS), F32)
    for i in range(PER_STEP):
        each = SLOTS // DIGIT
        one = [target[j : j + 1] for j in range(i * each, (i + 1) * each)]
        one = jnp.concatenate(one + [blank], axis=1)
        out_ref[i, SLOTS : SLOTS + 8] = jnp.broadcast_to(one, (8, width)).astype(BF16)


def later_prep(slot_ref, points_ref, out_ref, low):
    step = pl.program_id(0)

    @pl.when(step == 0)
    def _():
        low[...] = low_digits(slot_ref[...])

    rows = PER_STEP * SLOTS
    pick = pick_rows(slot_ref[...], low[...], step * rows, rows)
    moved = jnp.dot(pick, points_ref[...], preferred_element_type=F32)
    out_ref[...] = moved.astype(BF16).reshape(out_ref.shape)


def prepare(block_row, final_row, points, start, width, slot_row):
    npts = points.shape[0]
    steps = DESTS // PER_STEP
    column = start // width
    whole = pl.BlockSpec((1, npts), lambda i: (0, 0))
    point_spec = pl.BlockSpec((npts, width), lambda i: (0, column))
    tall = SLOTS if slot_row is not None else SLOTS + 8
    out_spec = pl.BlockSpec((PER_STEP, tall, width), lambda i: (i, 0, 0))
    out_shape = jax.ShapeDtypeStruct((DESTS, tall, width), BF16)
    cost = pl.CostEstimate(
        flops=2 * DESTS * SLOTS * npts * width,
        bytes_accessed=2 * width * (npts + DESTS * SLOTS),
        transcendentals=0,
    )
    if slot_row is not None:
        return pl.pallas_call(
            later_prep,
            grid=(steps,),
            in_specs=[whole, point_spec],
            out_specs=out_spec,
            out_shape=out_shape,
            scratch_shapes=[pltpu.VMEM((DIGIT, npts), BF16)],
            cost_estimate=cost,
        )(slot_row, points)
    return pl.pallas_call(
        first_prep,
        grid=(steps,),
        in_specs=[whole, whole, point_spec],
        out_specs=(out_spec, whole),
        out_shape=(out_shape, jax.ShapeDtypeStruct((1, npts), jnp.int32)),
        scratch_shapes=[
            pltpu.VMEM((1, npts), jnp.int32),
            pltpu.VMEM((DIGIT, npts), BF16),
            pltpu.VMEM((DESTS * SLOTS // DIGIT, DIGIT), F32),
        ],
        cost_estimate=cost,
    )(block_row, final_row, points)


def work_kernel(first, last, me_ref, *refs):
    refs = list(refs)
    rows_ref, target_ref = refs[:2]
    piece_refs = refs[2 : 3 + NZ]
    part_ref = None if first else refs[3 + NZ]
    far, half = NZ // 2, BS // 2
    sum_refs, result_ref, tables, packs = refs[-NZ - 3 : -3], refs[-3], refs[-2], refs[-1]
    places = [
        lax.rem(me_ref[0] - (pl.program_id(0) * PAIR + b) + NZ, NZ) for b in range(PAIR)
    ]
    for b in range(PAIR):
        for i in range(NZ):

            @pl.when(places[b] == i)
            def _(b=b, i=i):
                if i == far:
                    tables[b, :half] = piece_refs[far][...]
                    tables[b, half:] = piece_refs[far + 1][...]
                else:
                    tables[b] = piece_refs[i if i < far else i + 1][...]

    for b in range(PAIR):
        rows = rows_ref[:, b * MOST : (b + 1) * MOST, :].reshape(DESTS * MOST, rows_ref.shape[-1])
        table = tables[b]
        onehot = jnp.where(
            lax.broadcasted_iota(jnp.int32, (BS, DESTS * MOST), 0) == target_ref[b], 1.0, 0.0
        ).astype(BF16)
        sums = jnp.dot(onehot, rows, preferred_element_type=F32)
        packs[b, 0:BS] = sums.astype(BF16)
        if first:
            ones = jnp.ones((8, DESTS * MOST), BF16)
            count = nt_dot(ones, onehot)
            high = jnp.floor(count * (1.0 / 16.0))
            low = count - 16.0 * high
            which = lax.broadcasted_iota(jnp.int32, count.shape, 0)
            digits = jnp.where(which == 0, low, jnp.where(which == 1, high, 0.0))
            blank = jnp.zeros((8, sums.shape[1] - BS), F32)
            packs[b, BS : BS + 8] = jnp.concatenate([digits, blank], axis=1).astype(BF16)
        cross = nt_dot(rows, table)
        wide = rows.astype(F32)
        row_norm = jnp.sum(wide * wide, axis=1, keepdims=True)
        tall = table.astype(F32)
        cent_norm = jnp.sum(tall * tall, axis=1, keepdims=True)
        cent_norm = jnp.transpose(jnp.broadcast_to(cent_norm, (BS, 128)))[0:1]
        total = row_norm - 2.0 * cross + cent_norm
        if not first:
            total = total + part_ref[b]
        if last:
            total = (total * (1.0 / 1024.0)).astype(BF16)
            result_ref[:, b * MOST : (b + 1) * MOST, :] = total.reshape(DESTS, MOST, BS)
        else:
            result_ref[b] = total
    for b in range(PAIR):
        for i in range(NZ):

            @pl.when(places[b] == i)
            def _(b=b, i=i):
                sum_refs[i][...] = packs[b]


def block_work(me, rows, pieces, target, part, start, last):
    width = rows.shape[-1]
    first = part is None
    taken = DESTS * MOST
    tall = BS + 8 if first else BS
    row_spec = pl.BlockSpec((DESTS, PAIR * MOST, width), lambda k, me: (0, k, 0))
    part_spec = pl.BlockSpec((PAIR, taken, BS), lambda k, me: (k, 0, 0))
    in_specs = [row_spec, pl.BlockSpec((PAIR, 1, taken), lambda k, me: (k, 0, 0))]
    in_specs += [
        pl.BlockSpec((piece.shape[0], width), lambda k, me: (0, start // width))
        for piece in pieces
    ]
    operands = [rows, target, *pieces]
    if not first:
        in_specs.append(part_spec)
        operands.append(part)
    if last:
        result_spec = pl.BlockSpec((DESTS, PAIR * MOST, BS), lambda k, me: (0, k, 0))
        result_shape = jax.ShapeDtypeStruct((DESTS, SLOTS, BS), BF16)
    else:
        result_spec = part_spec
        result_shape = jax.ShapeDtypeStruct((NZ, taken, BS), F32)
    return pl.pallas_call(
        functools.partial(work_kernel, first, last),
        grid_spec=pltpu.PrefetchScalarGridSpec(
            num_scalar_prefetch=1,
            grid=(NZ // PAIR,),
            in_specs=in_specs,
            out_specs=(pl.BlockSpec((tall, width), lambda k, me: (0, 0)),) * NZ + (result_spec,),
            scratch_shapes=[
                pltpu.VMEM((PAIR, BS, width), BF16),
                pltpu.VMEM((PAIR, tall, width), BF16),
            ],
        ),
        out_shape=(jax.ShapeDtypeStruct((tall, width), BF16),) * NZ + (result_shape,),
        compiler_params=pltpu.CompilerParams(vmem_limit_bytes=None if last else WHOLE),
        cost_estimate=pl.CostEstimate(
            flops=4 * NZ * taken * BS * width,
            bytes_accessed=2 * width * NZ * (taken + 2 * BS) + 8 * NZ * taken * BS,
            transcendentals=0,
        ),
    )(me, *operands)


def return_kernel(slot_ref, returned_ref, out_ref):
    rows = out_ref.shape[0]
    lane = 128
    slot = jnp.transpose(jnp.broadcast_to(slot_ref[...].astype(F32), (lane, rows)))
    slot = slot.astype(jnp.int32)
    hit = slot % lane == lax.broadcasted_iota(jnp.int32, (rows, lane), 1)
    high = jnp.where(hit, slot // lane, -1).astype(F32).astype(BF16)
    total = jnp.zeros(out_ref.shape, F32)
    part = 1024
    for at in range(0, returned_ref.shape[0], part):
        pick = [mask(high == jnp.asarray(i // lane, BF16)) for i in range(at, at + part, lane)]
        pick = jnp.concatenate(pick, axis=1)
        total += jnp.dot(pick, returned_ref[at : at + part], preferred_element_type=F32)
    out_ref[...] = total.astype(BF16)


def pick_back(slot_row, returned):
    npts = slot_row.shape[1]
    rows = 512
    return pl.pallas_call(
        return_kernel,
        grid=(npts // rows,),
        in_specs=[
            pl.BlockSpec((1, rows), lambda i: (0, i)),
            pl.BlockSpec(returned.shape, lambda i: (0, 0)),
        ],
        out_specs=pl.BlockSpec((rows, BS), lambda i: (i, 0)),
        out_shape=jax.ShapeDtypeStruct((npts, BS), BF16),
        compiler_params=pltpu.CompilerParams(vmem_limit_bytes=GRANT),
        cost_estimate=pl.CostEstimate(
            flops=2 * npts * returned.shape[0] * BS,
            bytes_accessed=2 * BS * (npts + returned.shape[0]),
            transcendentals=0,
        ),
    )(slot_row, returned)


def exchange(values, axes):
    return lax.all_to_all(values, axes, split_axis=0, concat_axis=0, tiled=True)


def pass_on(values, distance):
    return lax.ppermute(values, "z", [(i, (i + distance) % NZ) for i in range(NZ)])


def gather_table(own):
    up, down, below, above = own, own, [], []
    for _ in range(1, NZ // 2):
        up, down = pass_on(up, 1), pass_on(down, -1)
        below.append(up)
        above.append(down)
    half = BS // 2
    far = [pass_on(up[:half], 1), pass_on(down[half:], -1)]
    return [own, *below, *far, *reversed(above)]


def sum_over_planes(sums):
    total = sums[0].astype(F32)
    for k in sorted(range(1, NZ), key=lambda k: -min(k, NZ - k)):
        total = total + pass_on(sums[k], -k).astype(F32)
    return total


def shards(points, blocks, finals, centroids):
    npts, _ = points.shape
    group = lax.axis_index("x") * NC + lax.axis_index("c")
    me = lax.axis_index("z").astype(jnp.int32).reshape(1)
    own = lax.dynamic_slice_in_dim(centroids, group * BS, BS, 0)
    pieces = gather_table(own)

    block_row = blocks.reshape(1, npts)
    final_row = finals.reshape(1, npts)
    last = len(WIDTHS) - 1
    starts = [sum(WIDTHS[:i]) for i in range(last + 1)]
    arrived, slot_row = [], None
    for i, size in enumerate(WIDTHS):
        sent = prepare(block_row, final_row, points, starts[i], size, slot_row)
        if i == 0:
            sent, slot_row = sent
        arrived.append(exchange(sent, PLANE))
    target = arrived[0][:, SLOTS, :SLOTS].astype(jnp.int32) - 1
    target = jnp.transpose(target.reshape(DESTS, NZ, MOST), (1, 0, 2))
    target = target.reshape(NZ, 1, DESTS * MOST)
    part, shares = None, []
    for i in range(last + 1):
        *sums, part = block_work(
            me, arrived[i], pieces, target, part, starts[i], i == last
        )
        shares.append(sum_over_planes(sums))
    returned = exchange(part, PLANE).reshape(DESTS * SLOTS, BS)
    distances = pick_back(slot_row, returned)

    counts = shares[0][BS, :BS] + 16.0 * shares[0][BS + 1, :BS]
    total = jnp.concatenate([s[:BS] for s in shares], axis=1)
    fresh = (total + own.astype(F32)) / (counts + 1.0)[:, None]
    fresh = lax.all_to_all(fresh.astype(BF16), ("x", "c"), split_axis=1, concat_axis=0, tiled=True)
    return distances, fresh.astype(F32)


def solution(mesh):
    split = Mesh(mesh.devices.reshape(NX, NC, NZ, NY), ("x", "c", "z", "y"))
    every = ("x", "c", "z", "y")
    placed = (P(every, None), P(every, None), P(every), P(("z", "y"), None))
    return jax.shard_map(
        shards,
        mesh=split,
        in_specs=placed,
        out_specs=(P(every, None), P(("z", "y"), ("x", "c"))),
        check_vma=False,
    )
```

```python
import functools

import jax
import jax.numpy as jnp
from jax import lax
from jax.experimental import pallas as pl
from jax.experimental.pallas import tpu as pltpu
from jax.sharding import Mesh
from jax.sharding import PartitionSpec as P

BS = 256
MOST = 16
NX, NC, NZ, NY = 4, 2, 8, 4
NG = NX * NC
NB = NZ * NY * NG
DESTS = NG * NY
SLOTS = NZ * MOST
WIDTHS = (384, 384, 256)
PLANE = ("x", "c", "y")
DIGIT = 64
GRANT = 32 * 2**20
WHOLE = 67043328
PAIR = 2
PER_STEP = 8
F32, BF16 = jnp.float32, jnp.bfloat16


def mask(where):
    return jnp.where(where, jnp.ones((), BF16), jnp.zeros((), BF16))


def nt_dot(a, b):
    return lax.dot_general(a, b, (((1,), (1,)), ((), ())), preferred_element_type=F32)


def slots_of(block_row):
    npts = block_row.shape[1]
    piece = 128
    row = lax.broadcasted_iota(jnp.int32, (piece, 2 * piece), 0)
    column = lax.broadcasted_iota(jnp.int32, (piece, 2 * piece), 1)
    before = jnp.where((row < column) | (column >= piece), 1.0, 0.0).astype(BF16)
    carry = jnp.zeros((NB, piece), F32)
    ranks = []
    for i in range(npts // piece):
        part = block_row[:, i * piece : (i + 1) * piece]
        member = lax.broadcasted_iota(jnp.int32, (NB, piece), 0) == part
        ones = jnp.where(member, 1.0, 0.0)
        seen = jnp.dot(ones.astype(BF16), before, preferred_element_type=F32)
        ranks.append(jnp.sum(ones * (seen[:, :piece] + carry), axis=0, keepdims=True))
        carry = carry + seen[:, piece:]
    rank = jnp.concatenate(ranks, axis=1).astype(jnp.int32)
    zz = block_row // (NY * NG)
    yy = (block_row // NG) % NY
    gg = block_row % NG
    return ((gg * NY + yy) * NZ + zz) * MOST + rank


def low_digits(slots):
    line = lax.broadcasted_iota(jnp.int32, (DIGIT, slots.shape[1]), 0)
    return jnp.where(line == slots % DIGIT, 1.0, 0.0).astype(BF16)


def pick_rows(slots, low, base, rows):
    npts = slots.shape[1]
    line = lax.broadcasted_iota(jnp.int32, (rows // DIGIT, npts), 0)
    high = jnp.where(line + base // DIGIT == slots // DIGIT, 1.0, 0.0)
    parts = []
    for i in range(rows // DIGIT):
        one = jnp.broadcast_to(high[i : i + 1], (16, npts)).astype(BF16)
        parts.append(low * jnp.concatenate([one] * (DIGIT // 16), axis=0))
    return jnp.concatenate(parts, axis=0)


def first_prep(block_ref, final_ref, points_ref, out_ref, slot_ref, slots, low, targets):
    step = pl.program_id(0)

    @pl.when(step == 0)
    def _():
        found = slots_of(block_ref[...])
        slots[...] = found
        slot_ref[...] = found
        low[...] = low_digits(found)
        line = lax.broadcasted_iota(jnp.int32, (DESTS * SLOTS // DIGIT, found.shape[1]), 0)
        high = jnp.where(line == found // DIGIT, (final_ref[...] + 1).astype(F32), 0.0)
        targets[...] = nt_dot(high.astype(BF16), low[...])

    rows = PER_STEP * SLOTS
    width = points_ref.shape[1]
    pick = pick_rows(slots[...], low[...], step * rows, rows)
    moved = jnp.dot(pick, points_ref[...], preferred_element_type=F32)
    out_ref[:, 0:SLOTS] = moved.astype(BF16).reshape(PER_STEP, SLOTS, width)
    digits = rows // DIGIT
    target = targets[pl.ds(pl.multiple_of(step * digits, digits), digits)]
    blank = jnp.zeros((1, width - SLOTS), F32)
    for i in range(PER_STEP):
        each = SLOTS // DIGIT
        one = [target[j : j + 1] for j in range(i * each, (i + 1) * each)]
        one = jnp.concatenate(one + [blank], axis=1)
        out_ref[i, SLOTS : SLOTS + 8] = jnp.broadcast_to(one, (8, width)).astype(BF16)


def later_prep(slot_ref, points_ref, out_ref, low):
    step = pl.program_id(0)

    @pl.when(step == 0)
    def _():
        low[...] = low_digits(slot_ref[...])

    rows = out_ref.shape[0] * SLOTS
    pick = pick_rows(slot_ref[...], low[...], step * rows, rows)
    moved = jnp.dot(pick, points_ref[...], preferred_element_type=F32)
    out_ref[...] = moved.astype(BF16).reshape(out_ref.shape)


def prepare(block_row, final_row, points, start, width, slot_row):
    npts = points.shape[0]
    per = PER_STEP if slot_row is None else PER_STEP // 2
    steps = DESTS // per
    column = start // width
    whole = pl.BlockSpec((1, npts), lambda i: (0, 0))
    point_spec = pl.BlockSpec((npts, width), lambda i: (0, column))
    tall = SLOTS if slot_row is not None else SLOTS + 8
    out_spec = pl.BlockSpec((per, tall, width), lambda i: (i, 0, 0))
    out_shape = jax.ShapeDtypeStruct((DESTS, tall, width), BF16)
    cost = pl.CostEstimate(
        flops=2 * DESTS * SLOTS * npts * width,
        bytes_accessed=2 * width * (npts + DESTS * SLOTS),
        transcendentals=0,
    )
    if slot_row is not None:
        return pl.pallas_call(
            later_prep,
            grid=(steps,),
            in_specs=[whole, point_spec],
            out_specs=out_spec,
            out_shape=out_shape,
            scratch_shapes=[pltpu.VMEM((DIGIT, npts), BF16)],
            cost_estimate=cost,
        )(slot_row, points)
    return pl.pallas_call(
        first_prep,
        grid=(steps,),
        in_specs=[whole, whole, point_spec],
        out_specs=(out_spec, whole),
        out_shape=(out_shape, jax.ShapeDtypeStruct((1, npts), jnp.int32)),
        scratch_shapes=[
            pltpu.VMEM((1, npts), jnp.int32),
            pltpu.VMEM((DIGIT, npts), BF16),
            pltpu.VMEM((DESTS * SLOTS // DIGIT, DIGIT), F32),
        ],
        cost_estimate=cost,
    )(block_row, final_row, points)


def work_kernel(first, last, me_ref, *refs):
    refs = list(refs)
    rows_ref, target_ref = refs[:2]
    piece_refs = refs[2 : 3 + NZ]
    part_ref = None if first else refs[3 + NZ]
    far, half = NZ // 2, BS // 2
    sum_refs, result_ref, tables, packs = refs[-NZ - 3 : -3], refs[-3], refs[-2], refs[-1]
    places = [
        lax.rem(me_ref[0] - (pl.program_id(0) * PAIR + b) + NZ, NZ) for b in range(PAIR)
    ]
    for b in range(PAIR):
        for i in range(NZ):

            @pl.when(places[b] == i)
            def _(b=b, i=i):
                if i == far:
                    tables[b, :half] = piece_refs[far][...]
                    tables[b, half:] = piece_refs[far + 1][...]
                else:
                    tables[b] = piece_refs[i if i < far else i + 1][...]

    for b in range(PAIR):
        rows = rows_ref[:, b * MOST : (b + 1) * MOST, :].reshape(DESTS * MOST, rows_ref.shape[-1])
        table = tables[b]
        onehot = jnp.where(
            lax.broadcasted_iota(jnp.int32, (BS, DESTS * MOST), 0) == target_ref[b], 1.0, 0.0
        ).astype(BF16)
        sums = jnp.dot(onehot, rows, preferred_element_type=F32)
        packs[b, 0:BS] = sums.astype(BF16)
        if first:
            ones = jnp.ones((8, DESTS * MOST), BF16)
            count = nt_dot(ones, onehot)
            high = jnp.floor(count * (1.0 / 16.0))
            low = count - 16.0 * high
            which = lax.broadcasted_iota(jnp.int32, count.shape, 0)
            digits = jnp.where(which == 0, low, jnp.where(which == 1, high, 0.0))
            blank = jnp.zeros((8, sums.shape[1] - BS), F32)
            packs[b, BS : BS + 8] = jnp.concatenate([digits, blank], axis=1).astype(BF16)
        cross = nt_dot(rows, table)
        wide = rows.astype(F32)
        row_norm = jnp.sum(wide * wide, axis=1, keepdims=True)
        tall = table.astype(F32)
        cent_norm = jnp.sum(tall * tall, axis=1, keepdims=True)
        cent_norm = jnp.transpose(jnp.broadcast_to(cent_norm, (BS, 128)))[0:1]
        total = row_norm - 2.0 * cross + cent_norm
        if not first:
            total = total + part_ref[b]
        if last:
            total = (total * (1.0 / 1024.0)).astype(BF16)
            result_ref[:, b * MOST : (b + 1) * MOST, :] = total.reshape(DESTS, MOST, BS)
        else:
            result_ref[b] = total
    for b in range(PAIR):
        for i in range(NZ):

            @pl.when(places[b] == i)
            def _(b=b, i=i):
                sum_refs[i][...] = packs[b]


def block_work(me, rows, pieces, target, part, start, last):
    width = rows.shape[-1]
    first = part is None
    taken = DESTS * MOST
    tall = BS + 8 if first else BS
    row_spec = pl.BlockSpec((DESTS, PAIR * MOST, width), lambda k, me: (0, k, 0))
    part_spec = pl.BlockSpec((PAIR, taken, BS), lambda k, me: (k, 0, 0))
    in_specs = [row_spec, pl.BlockSpec((PAIR, 1, taken), lambda k, me: (k, 0, 0))]
    in_specs += [
        pl.BlockSpec((piece.shape[0], width), lambda k, me: (0, start // width))
        for piece in pieces
    ]
    operands = [rows, target, *pieces]
    if not first:
        in_specs.append(part_spec)
        operands.append(part)
    if last:
        result_spec = pl.BlockSpec((DESTS, PAIR * MOST, BS), lambda k, me: (0, k, 0))
        result_shape = jax.ShapeDtypeStruct((DESTS, SLOTS, BS), BF16)
    else:
        result_spec = part_spec
        result_shape = jax.ShapeDtypeStruct((NZ, taken, BS), F32)
    return pl.pallas_call(
        functools.partial(work_kernel, first, last),
        grid_spec=pltpu.PrefetchScalarGridSpec(
            num_scalar_prefetch=1,
            grid=(NZ // PAIR,),
            in_specs=in_specs,
            out_specs=(pl.BlockSpec((tall, width), lambda k, me: (0, 0)),) * NZ + (result_spec,),
            scratch_shapes=[
                pltpu.VMEM((PAIR, BS, width), BF16),
                pltpu.VMEM((PAIR, tall, width), BF16),
            ],
        ),
        out_shape=(jax.ShapeDtypeStruct((tall, width), BF16),) * NZ + (result_shape,),
        compiler_params=pltpu.CompilerParams(vmem_limit_bytes=None if last else WHOLE),
        cost_estimate=pl.CostEstimate(
            flops=4 * NZ * taken * BS * width,
            bytes_accessed=2 * width * NZ * (taken + 2 * BS) + 8 * NZ * taken * BS,
            transcendentals=0,
        ),
    )(me, *operands)


def return_kernel(slot_ref, returned_ref, out_ref):
    rows = out_ref.shape[0]
    lane = 128
    slot = jnp.transpose(jnp.broadcast_to(slot_ref[...].astype(F32), (lane, rows)))
    slot = slot.astype(jnp.int32)
    hit = slot % lane == lax.broadcasted_iota(jnp.int32, (rows, lane), 1)
    high = jnp.where(hit, slot // lane, -1).astype(F32).astype(BF16)
    total = jnp.zeros(out_ref.shape, F32)
    part = 1024
    for at in range(0, returned_ref.shape[0], part):
        pick = [mask(high == jnp.asarray(i // lane, BF16)) for i in range(at, at + part, lane)]
        pick = jnp.concatenate(pick, axis=1)
        total += jnp.dot(pick, returned_ref[at : at + part], preferred_element_type=F32)
    out_ref[...] = total.astype(BF16)


def pick_back(slot_row, returned):
    npts = slot_row.shape[1]
    rows = 512
    return pl.pallas_call(
        return_kernel,
        grid=(npts // rows,),
        in_specs=[
            pl.BlockSpec((1, rows), lambda i: (0, i)),
            pl.BlockSpec(returned.shape, lambda i: (0, 0)),
        ],
        out_specs=pl.BlockSpec((rows, BS), lambda i: (i, 0)),
        out_shape=jax.ShapeDtypeStruct((npts, BS), BF16),
        compiler_params=pltpu.CompilerParams(vmem_limit_bytes=GRANT),
        cost_estimate=pl.CostEstimate(
            flops=2 * npts * returned.shape[0] * BS,
            bytes_accessed=2 * BS * (npts + returned.shape[0]),
            transcendentals=0,
        ),
    )(slot_row, returned)


def exchange(values, axes):
    return lax.all_to_all(values, axes, split_axis=0, concat_axis=0, tiled=True)


def pass_on(values, distance):
    return lax.ppermute(values, "z", [(i, (i + distance) % NZ) for i in range(NZ)])


def gather_table(own):
    up, down, below, above = own, own, [], []
    for _ in range(1, NZ // 2):
        up, down = pass_on(up, 1), pass_on(down, -1)
        below.append(up)
        above.append(down)
    half = BS // 2
    far = [pass_on(up[:half], 1), pass_on(down[half:], -1)]
    return [own, *below, *far, *reversed(above)]


def sum_over_planes(sums):
    total = sums[0].astype(F32)
    for k in sorted(range(1, NZ), key=lambda k: -min(k, NZ - k)):
        total = total + pass_on(sums[k], -k).astype(F32)
    return total


def shards(points, blocks, finals, centroids):
    npts, _ = points.shape
    group = lax.axis_index("x") * NC + lax.axis_index("c")
    me = lax.axis_index("z").astype(jnp.int32).reshape(1)
    own = lax.dynamic_slice_in_dim(centroids, group * BS, BS, 0)
    pieces = gather_table(own)

    block_row = blocks.reshape(1, npts)
    final_row = finals.reshape(1, npts)
    last = len(WIDTHS) - 1
    starts = [sum(WIDTHS[:i]) for i in range(last + 1)]
    arrived, slot_row = [], None
    for i, size in enumerate(WIDTHS):
        sent = prepare(block_row, final_row, points, starts[i], size, slot_row)
        if i == 0:
            sent, slot_row = sent
        arrived.append(exchange(sent, PLANE))
    target = arrived[0][:, SLOTS, :SLOTS].astype(jnp.int32) - 1
    target = jnp.transpose(target.reshape(DESTS, NZ, MOST), (1, 0, 2))
    target = target.reshape(NZ, 1, DESTS * MOST)
    part, shares = None, []
    for i in range(last + 1):
        *sums, part = block_work(
            me, arrived[i], pieces, target, part, starts[i], i == last
        )
        shares.append(sum_over_planes(sums))
    returned = exchange(part, PLANE).reshape(DESTS * SLOTS, BS)
    distances = pick_back(slot_row, returned)

    counts = shares[0][BS, :BS] + 16.0 * shares[0][BS + 1, :BS]
    fresh = []
    for i, share in enumerate(shares):
        before = own[:, starts[i] : starts[i] + WIDTHS[i]].astype(F32)
        fresh.append(((share[:BS] + before) / (counts + 1.0)[:, None]).astype(BF16))
    fresh = jnp.concatenate([*lax.optimization_barrier(fresh[:last]), fresh[last]], axis=1)
    fresh = lax.all_to_all(fresh, ("x", "c"), split_axis=1, concat_axis=0, tiled=True)
    return distances, fresh.astype(F32)


def solution(mesh):
    split = Mesh(mesh.devices.reshape(NX, NC, NZ, NY), ("x", "c", "z", "y"))
    every = ("x", "c", "z", "y")
    placed = (P(every, None), P(every, None), P(every), P(("z", "y"), None))
    return jax.shard_map(
        shards,
        mesh=split,
        in_specs=placed,
        out_specs=(P(every, None), P(("z", "y"), ("x", "c"))),
        check_vma=False,
    )
```
